512 devices in a mesh: tm: 128 (over z, y, core), pair: 4 (over x).
Axes of the slice: x: 4, y: 8, z: 8, core: 2. Of those that a mesh axis runs over, the one named last changes fastest.
Arguments:
- x_series: float32 [128, 524288], P('pair', 'tm'), may hold values from -6 to 6
- y_series: float32 [128, 524288], P('pair', 'tm'), may hold values from -6 to 6
Outputs:
- correlation: float32 [128, 512], P('tm', 'pair')
The draws below stay inside these ranges and needn't reach their ends.
All inputs are finite; a program needn't handle non-finite values.
Results may differ from the reference program's by a relative error of at most 0.000082.
Values sent between devices are 32-bit elements; how exact they have to be, the bound alone decides.
A program may use at most 64 MiB of HBM per device.

```python
import math
import jax
import jax.numpy as jnp
from jax import lax

L = 512
PAIRS = 128
NT = 524288


def block_scale(own_key, extent, cuts, low, largest):
    level = 1.0
    for axis_at, parts in cuts:
        steps = jax.random.uniform(jax.random.fold_in(jax.random.fold_in(own_key, 6), axis_at), (parts,), jnp.float32, low / len(cuts), largest / len(cuts))
        level = level * jnp.repeat(jnp.exp(steps), extent[axis_at] // parts).reshape((-1,) + (1,) * (len(extent) - 1 - axis_at))
    return level


def bell_draw(stream_key, dims, width, most, cuts=(), held_as=jnp.bfloat16):
    result = jax.random.normal(stream_key, dims, jnp.float32) * width
    if len(cuts) > 0:
        result = block_scale(stream_key, dims, cuts, -0.22, 0.18) * result
    return jnp.clip(result, min=-most, max=most).astype(held_as)


def setup_inputs(seed: int = 0) -> dict:
    splits = jax.random.split(jax.random.key(seed), 3)
    return {
        "x_series": bell_draw(splits[0], (PAIRS, NT), 1.0, 6.0, ((0, 4), (1, 128)), jnp.float32),
        "y_series": bell_draw(splits[1], (PAIRS, NT), 1.0, 6.0, ((0, 4), (1, 128)), jnp.float32),
    }


def lag_products(series, extended):
    block_len = min(128, L)
    pair_count, length = series.shape
    block_rows = length // block_len
    left_rows = series.reshape(pair_count, block_rows, block_len)
    pieces = [extended[:, offset * block_len:offset * block_len + length].reshape(pair_count, block_rows, block_len) for offset in range(L // block_len + 1)]
    right_rows = jnp.concatenate(pieces, axis=2)
    grams = jnp.einsum('pbi,pbj->pij', left_rows, right_rows, precision=lax.Precision.HIGHEST, preferred_element_type=jnp.float32)
    span_cols = L + block_len
    flattened = grams.reshape(pair_count, block_len * span_cols)
    flattened = jnp.pad(flattened, ((0, 0), (0, block_len)))
    skewed = flattened.reshape(pair_count, block_len, span_cols + 1)
    return lax.optimization_barrier(jnp.sum(skewed[:, :, :L], axis=1))

def per_block(members):
    return lag_products(members[0], members[1])

def reference(x_series, y_series):
    extended = jnp.pad(y_series, ((0, 0), (0, L)))
    block_count = PAIRS // 8
    totals = lax.map(per_block, (x_series.reshape(block_count, 8, NT), extended.reshape(block_count, 8, NT + L)))
    totals = totals.reshape(PAIRS, L)
    return totals * (1.0 / math.sqrt(NT))
```

```python
import functools
import math

import jax
import jax.numpy as jnp
import ml_dtypes
import numpy as np
from jax import lax
from jax.experimental import pallas as pl
from jax.experimental.pallas import tpu as pltpu
from jax.sharding import PartitionSpec as P

L = 512
BLK = 256
N = 768
F = N // 2
MESH = pl.DeviceIdType.MESH


def halves(array):
    high = array.astype(ml_dtypes.bfloat16)
    low = (array - high.astype(np.float64)).astype(ml_dtypes.bfloat16)
    return high, low


@functools.cache
def tables(total):
    theta = 2 * np.pi * (np.arange(F) + 0.5) / N
    sample, lag = np.arange(BLK), np.arange(L)
    forward = np.concatenate(
        [np.cos(np.outer(sample, theta)), np.sin(np.outer(sample, theta))], axis=1
    )
    backward = np.concatenate(
        [np.cos(np.outer(theta, lag)), -np.sin(np.outer(theta, lag))], axis=0
    ) * (2.0 / N / math.sqrt(total))
    high, low = halves(forward)
    fwd = np.concatenate([high, high, low], axis=0)
    high, low = halves(backward)
    bwd = np.concatenate([high, high, low], axis=0)
    once, twice = np.exp(-1j * theta * BLK), np.exp(-2j * theta * BLK)
    turns = np.zeros((8, F), np.float32)
    turns[0], turns[1], turns[2], turns[3] = once.real, once.imag, twice.real, twice.imag
    return fwd, bwd, turns


def split_in(value, ref, row, width):
    high = value.astype(jnp.bfloat16)
    low = (value - high.astype(jnp.float32)).astype(jnp.bfloat16)
    rows = value.shape[0]
    ref[row : row + rows, 0:width] = high
    ref[row : row + rows, width : 2 * width] = low
    ref[row : row + rows, 2 * width : 3 * width] = high


def kernel(
    sizes, x_hbm, y_hbm, fwd_hbm, bwd_hbm, turns_hbm, out_ref,
    xv, yv, head, fwd, bwd, turns, parts, fx, fy, res, rparts,
    send_a, recv_a, send_b, recv_b,
    load_sem, halo_sem, sa_sem, ra_sem, sb_sem, rb_sem,
):
    zs, ys, xs = sizes
    pairs, length = xv.shape
    blocks = length // BLK
    extra = L // BLK
    group = 2 * ys
    depth = zs // xs
    tm, mx = lax.axis_index("tm"), lax.axis_index("pair")
    mz, mg = tm // group, tm % group
    my, mc = mg // 2, mg % 2
    steps = [ys // 2]
    for d in range(ys // 2 - 1, 0, -1):
        steps += [d, ys - d]
    peers = [(d, c) for d in steps for c in (0, 1)] + [(0, 1)]

    def peer(d, c):
        return ((my + d) % ys) * 2 + (mc + c) % 2

    loads = [
        pltpu.make_async_copy(x_hbm, xv, load_sem.at[0]),
        pltpu.make_async_copy(fwd_hbm, fwd, load_sem.at[1]),
        pltpu.make_async_copy(y_hbm, yv, load_sem.at[2]),
        pltpu.make_async_copy(turns_hbm, turns, load_sem.at[3]),
        pltpu.make_async_copy(bwd_hbm, bwd, load_sem.at[4]),
    ]
    for load in loads:
        load.start()

    barrier = pltpu.get_barrier_semaphore()
    last = zs * group - 1

    @pl.when(tm < last)
    def _():
        pl.semaphore_signal(
            barrier, inc=1, device_id=(tm + 1, mx), device_id_type=MESH
        )

    source_x = mz // depth
    for z in range(zs):

        @pl.when(jnp.logical_or(source_x != mx, z != mz))
        def _():
            pl.semaphore_signal(
                barrier, inc=1, device_id=(z * group + mg, source_x), device_id_type=MESH
            )

    for d, c in peers:
        pl.semaphore_signal(
            barrier, inc=1, device_id=(mz * group + peer(d, c), mx), device_id_type=MESH
        )

    loads[0].wait()
    for j in range(blocks):
        split_in(xv[:, j * BLK : (j + 1) * BLK], parts, j * pairs, BLK)
    loads[1].wait()
    fx[...] = jnp.dot(
        parts[0 : blocks * pairs, :], fwd[...], preferred_element_type=jnp.float32
    )

    own = jnp.where(source_x == mx, 1, 0)
    wanted = (group - 1) + depth * xs - own + jnp.where(tm > 0, 1, 0)
    pl.semaphore_wait(barrier, wanted)
    loads[2].wait()
    halo = pltpu.make_async_remote_copy(
        src_ref=yv.at[:, 0:L],
        dst_ref=head,
        send_sem=halo_sem.at[0],
        recv_sem=halo_sem.at[1],
        device_id=(jnp.maximum(tm - 1, 0), mx),
        device_id_type=MESH,
    )

    @pl.when(tm > 0)
    def _():
        halo.start()

    @pl.when(tm == last)
    def _():
        head[...] = jnp.zeros_like(head)

    for j in range(blocks):
        split_in(yv[:, j * BLK : (j + 1) * BLK], parts, j * pairs, BLK)
    fy[0 : blocks * pairs, :] = jnp.dot(
        parts[0 : blocks * pairs, :], fwd[...], preferred_element_type=jnp.float32
    )
    loads[3].wait()

    def take(ref, block, at, c):
        rows = pl.ds(pl.multiple_of(block * pairs + at, 8), 8)
        return ref[rows, c * 128 : (c + 1) * 128], ref[rows, F + c * 128 : F + (c + 1) * 128]

    def turn(which, c):
        lanes = slice(c * 128, (c + 1) * 128)
        real, imag = turns[2 * which : 2 * which + 1, lanes], turns[2 * which + 1 : 2 * which + 2, lanes]
        return real, imag

    def products(at, c, first, terms):
        xs_ = {i: take(fx, i, at, c) for i in sorted({i for i, _ in terms})} if not first else {}
        sums = {}
        for i, j in terms:
            cx, sx = xs_[i] if i in xs_ else take(fx, i, at, c)
            cy, sy = take(fy, j, at, c)
            real, imag = cx * cy + sx * sy, sx * cy - cx * sy
            if j - i in sums:
                a, b = sums[j - i]
                real, imag = real + a, imag + b
            sums[j - i] = (real, imag)
        total_real = total_imag = None
        for shift, (real, imag) in sums.items():
            if shift > 0:
                a, b = turn(shift - 1, c)
                real, imag = real * a - imag * b, real * b + imag * a
            total_real = real if total_real is None else total_real + real
            total_imag = imag if total_imag is None else total_imag + imag
        return total_real, total_imag

    near = [(i, i + s) for i in range(blocks) for s in range(extra + 1) if i + s < blocks]
    far = [(i, i + s) for i in range(blocks) for s in range(extra + 1) if i + s >= blocks]

    @pl.loop(0, pairs // 8)
    def _(g):
        at = pl.multiple_of(g * 8, 8)
        for c in range(F // 128):
            real, imag = products(at, c, True, near)
            res[pl.ds(at, 8), c * 128 : (c + 1) * 128] = real
            res[pl.ds(at, 8), F + c * 128 : F + (c + 1) * 128] = imag

    @pl.when(tm < last)
    def _():
        halo.wait_recv()

    for j in range(extra):
        split_in(head[:, j * BLK : (j + 1) * BLK], parts, j * pairs, BLK)
    fy[blocks * pairs : (blocks + extra) * pairs, :] = jnp.dot(
        parts[0 : extra * pairs, :], fwd[...], preferred_element_type=jnp.float32
    )
    for g in range(pairs // 8):
        for c in range(F // 128):
            real, imag = products(g * 8, c, False, far)
            res[g * 8 : g * 8 + 8, c * 128 : (c + 1) * 128] += real
            res[g * 8 : g * 8 + 8, F + c * 128 : F + (c + 1) * 128] += imag

    split_in(res[...], rparts, 0, N)
    loads[4].wait()
    lagged = jnp.dot(rparts[...], bwd[...], preferred_element_type=jnp.float32)
    for e in range(depth):
        for q in range(xs):
            send_a[:, e * xs + q, :] = lagged[
                e * group : (e + 1) * group, q * 128 : (q + 1) * 128
            ]

    def copy_a(at, slot):
        return pltpu.make_async_remote_copy(
            src_ref=send_a.at[at],
            dst_ref=recv_a.at[slot],
            send_sem=sa_sem.at[at],
            recv_sem=ra_sem.at[slot],
            device_id=(mz * group + at, mx),
            device_id_type=MESH,
        )

    for d, c in peers:
        copy_a(peer(d, c), mg).start()
    total = send_a[mg]
    for d, c in reversed(peers):
        at = peer(d, c)
        copy_a(at, at).wait_recv()
        total = total + recv_a[at]
    for i in range(depth * xs):
        send_b[i] = total[i : i + 1, :]

    def copy_b(i, slot):
        z, q = mx * depth + i // xs, i % xs
        return pltpu.make_async_remote_copy(
            src_ref=send_b.at[i],
            dst_ref=recv_b.at[slot],
            send_sem=sb_sem.at[i],
            recv_sem=rb_sem.at[slot],
            device_id=(z * group + mg, q),
            device_id_type=MESH,
        )

    def is_own(i):
        return jnp.logical_and(mx * depth + i // xs == mz, i % xs == mx)

    for i in range(depth * xs):

        @pl.when(jnp.logical_not(is_own(i)))
        def _():
            copy_b(i, mz).start()

        @pl.when(is_own(i))
        def _():
            recv_b[mz] = send_b[i]

    for z in range(zs):

        @pl.when(jnp.logical_or(source_x != mx, z != mz))
        def _():
            copy_b(0, z).wait_recv()

    value = recv_b[0]
    for z in range(1, zs):
        value = value + recv_b[z]
    out_ref[...] = value

    @pl.when(tm > 0)
    def _():
        halo.wait_send()

    for d, c in peers:
        copy_a(peer(d, c), mg).wait_send()
    for i in range(depth * xs):

        @pl.when(jnp.logical_not(is_own(i)))
        def _():
            copy_b(i, mz).wait_send()


def body(sizes, total, x_series, y_series):
    fwd, bwd, turns = tables(total)
    zs, ys, xs = sizes
    pairs, length = x_series.shape
    group, depth = 2 * ys, zs // xs
    blocks, extra = length // BLK, L // BLK
    f32, bf16 = jnp.float32, jnp.bfloat16
    dma = pltpu.SemaphoreType.DMA
    return pl.pallas_call(
        functools.partial(kernel, sizes),
        out_shape=jax.ShapeDtypeStruct((1, L // xs), f32),
        in_specs=[pl.BlockSpec(memory_space=pl.ANY)] * 5,
        out_specs=pl.BlockSpec(memory_space=pltpu.VMEM),
        scratch_shapes=[
            pltpu.VMEM((pairs, length), f32),
            pltpu.VMEM((pairs, length), f32),
            pltpu.VMEM((pairs, L), f32),
            pltpu.VMEM(fwd.shape, bf16),
            pltpu.VMEM(bwd.shape, bf16),
            pltpu.VMEM(turns.shape, f32),
            pltpu.VMEM((blocks * pairs, 3 * BLK), bf16),
            pltpu.VMEM((blocks * pairs, N), f32),
            pltpu.VMEM(((blocks + extra) * pairs, N), f32),
            pltpu.VMEM((pairs, N), f32),
            pltpu.VMEM((pairs, 3 * N), bf16),
            pltpu.VMEM((group, depth * xs, L // xs), f32),
            pltpu.VMEM((group, depth * xs, L // xs), f32),
            pltpu.VMEM((depth * xs, 1, L // xs), f32),
            pltpu.VMEM((zs, 1, L // xs), f32),
            dma((5,)),
            dma((2,)),
            dma((group,)),
            dma((group,)),
            dma((depth * xs,)),
            dma((zs,)),
        ],
        compiler_params=pltpu.CompilerParams(
            collective_id=0, has_side_effects=True
        ),
    )(x_series, y_series, jnp.asarray(fwd), jnp.asarray(bwd), jnp.asarray(turns))


def solution(mesh):
    sizes = (8, 8, mesh.shape["pair"])
    total = 524288
    return jax.shard_map(
        functools.partial(body, sizes, total),
        mesh=mesh,
        in_specs=(P("pair", "tm"), P("pair", "tm")),
        out_specs=P("tm", "pair"),
        check_vma=False,
    )
```

```python
import functools
import math

import jax
import jax.numpy as jnp
import ml_dtypes
import numpy as np
from jax import lax
from jax.experimental import pallas as pl
from jax.experimental.pallas import tpu as pltpu
from jax.sharding import PartitionSpec as P

L = 512
BLK = 128
N = 2 * BLK
MESH = pl.DeviceIdType.MESH


def halves(array):
    high = array.astype(ml_dtypes.bfloat16)
    low = (array - high.astype(np.float64)).astype(ml_dtypes.bfloat16)
    return high, low


@functools.cache
def tables():
    theta = 2 * np.pi * (np.arange(BLK) + 0.5) / N
    turns = np.outer(np.arange(BLK), theta)
    high, low = halves(np.concatenate([np.cos(turns), np.sin(turns)], axis=1))
    forward = np.stack([np.concatenate([high, high]), np.concatenate([low, low])])
    high, low = halves(np.concatenate([np.cos(turns.T), -np.sin(turns.T)]) * (2.0 / N))
    return forward, np.concatenate([high, low], axis=1)


def high_low(value):
    high = value.astype(jnp.bfloat16)
    return high, (value - high.astype(jnp.float32)).astype(jnp.bfloat16)


def kernel(
    sizes, x_hbm, y_hbm, fwd_hbm, bwd_hbm, out_ref,
    xv, yv, lead, head, fwd, bwd, parts, fx, fy, res, rparts, send, recv,
    load_sem, halo_sem, send_sem, recv_sem,
):
    zs, ys, xs = sizes
    pairs, length = xv.shape
    blocks, extra = length // BLK, L // BLK
    group = 2 * ys
    depth = zs // xs
    everyone = zs * group
    last = everyone - 1
    tm, mx = lax.axis_index("tm"), lax.axis_index("pair")
    mz, mg = tm // group, tm % group
    source_x = mz // depth
    own = jnp.where(source_x == mx, 1, 0)

    loads = [
        pltpu.make_async_copy(y_hbm.at[:, 0:L], lead, load_sem.at[0]),
        pltpu.make_async_copy(x_hbm, xv, load_sem.at[1]),
        pltpu.make_async_copy(fwd_hbm, fwd, load_sem.at[2]),
        pltpu.make_async_copy(y_hbm, yv, load_sem.at[3]),
        pltpu.make_async_copy(bwd_hbm, bwd, load_sem.at[4]),
    ]
    for load in loads:
        load.start()

    barrier = pltpu.get_barrier_semaphore()

    @pl.when(tm < last)
    def _():
        pl.semaphore_signal(barrier, inc=1, device_id=(tm + 1, mx), device_id_type=MESH)

    for step in range(1, everyone):
        other = lax.rem(tm + step, everyone)
        pl.semaphore_signal(barrier, inc=1, device_id=(other, source_x), device_id_type=MESH)

    @pl.when(own == 0)
    def _():
        pl.semaphore_signal(barrier, inc=1, device_id=(tm, source_x), device_id_type=MESH)

    def transform(value, at, into):
        count = value.shape[1] // BLK
        for j in range(count):
            high, low = high_low(value[:, j * BLK : (j + 1) * BLK])
            parts[j * pairs : (j + 1) * pairs, 0:BLK] = high
            parts[j * pairs : (j + 1) * pairs, BLK : 2 * BLK] = low
        rows = parts[0 : count * pairs, :]
        into[at * pairs : (at + count) * pairs, :] = jnp.dot(
            rows, fwd[0], preferred_element_type=jnp.float32
        ) + jnp.dot(rows, fwd[1], preferred_element_type=jnp.float32)

    loads[1].wait()
    loads[2].wait()
    transform(xv, 0, fx)

    loads[0].wait()
    pl.semaphore_wait(barrier, pairs * xs - own + jnp.where(tm > 0, 1, 0))
    halo = pltpu.make_async_remote_copy(
        src_ref=lead,
        dst_ref=head,
        send_sem=halo_sem.at[0],
        recv_sem=halo_sem.at[1],
        device_id=(jnp.maximum(tm - 1, 0), mx),
        device_id_type=MESH,
    )

    @pl.when(tm > 0)
    def _():
        halo.start()

    @pl.when(tm == last)
    def _():
        head[...] = jnp.zeros_like(head)

    loads[3].wait()
    transform(yv, 0, fy)

    lane = lax.broadcasted_iota(jnp.int32, (8, BLK), 1)
    sign = jnp.where(lane % 2 == 0, 1.0, -1.0).astype(jnp.float32)

    def take(ref, block, at):
        rows = pl.ds(pl.multiple_of(block * pairs + at, 8), 8)
        return ref[rows, 0:BLK], ref[rows, BLK : 2 * BLK]

    def products(at, first, past):
        sums = [None] * extra
        window = {}
        ahead = None
        for j in range(first, past):
            now = take(fy, j, at) if ahead is None else ahead
            ahead = take(fy, j + 1, at)
            window[j] = (now[0] - sign * ahead[1], now[1] + sign * ahead[0])
        terms = {}
        for q in range(extra):
            for b in range(blocks):
                if first <= b + q < past:
                    terms.setdefault(b, []).append(q)
        for b, lags in terms.items():
            cx, sx = take(fx, b, at)
            for q in lags:
                cz, sz = window[b + q]
                real, imag = cx * cz + sx * sz, sx * cz - cx * sz
                if sums[q] is not None:
                    real, imag = real + sums[q][0], imag + sums[q][1]
                sums[q] = (real, imag)
        return sums

    @pl.loop(0, pairs // 8)
    def _(g):
        at = pl.multiple_of(g * 8, 8)
        for q, (real, imag) in enumerate(products(at, 0, blocks - 1)):
            rows = pl.ds(pl.multiple_of(q * pairs + at, 8), 8)
            res[rows, 0:BLK] = real
            res[rows, BLK : 2 * BLK] = imag

    @pl.when(tm < last)
    def _():
        halo.wait_recv()

    transform(head, blocks, fy)
    for at in range(0, pairs, 8):
        for q, (real, imag) in enumerate(products(at, blocks - 1, blocks + extra - 1)):
            rows = slice(q * pairs + at, q * pairs + at + 8)
            for half, value in enumerate((real, imag)):
                columns = slice(half * BLK, (half + 1) * BLK)
                high, low = high_low(res[rows, columns] + value)
                rparts[rows, columns] = high.astype(jnp.float32)
                rparts[extra * pairs + q * pairs + at : extra * pairs + q * pairs + at + 8, columns] = low.astype(jnp.float32)

    loads[4].wait()
    both = jnp.dot(rparts[...].astype(jnp.bfloat16), bwd[...], preferred_element_type=jnp.float32)
    half = extra * pairs
    lagged = (both[0:half, 0:BLK] + both[0:half, BLK : 2 * BLK]) + (
        both[half:, 0:BLK] + both[half:, BLK : 2 * BLK]
    )
    send[...] = lagged.reshape(half, 1, BLK)

    def copy(row, q):
        return pltpu.make_async_remote_copy(
            src_ref=send.at[q * pairs + row],
            dst_ref=recv.at[tm],
            send_sem=send_sem,
            recv_sem=recv_sem,
            device_id=(mx * pairs + row, q),
            device_id_type=MESH,
        )

    order = [0]
    for d in range(1, ys // 2):
        order += [d, ys - d]
    order.append(ys // 2)
    for y in order:
        for e in range(depth):
            for c in (0, 1):
                row = e * group + y * 2 + c
                for step in range(1, xs):
                    copy(row, lax.rem(mx + step, xs)).start()

                @pl.when(mx * pairs + row != tm)
                def _():
                    copy(row, mx).start()

    @pl.when(own == 1)
    def _():
        recv[tm] = send[mx * pairs + (tm - mx * pairs)]

    def all_of(count):
        return pltpu.make_async_remote_copy(
            src_ref=send.at[pl.ds(0, count)],
            dst_ref=recv.at[pl.ds(0, count)],
            send_sem=send_sem,
            recv_sem=recv_sem,
            device_id=(tm, mx),
            device_id_type=MESH,
        )

    for own_too in (0, 1):

        @pl.when(own == own_too)
        def _():
            all_of(everyone - own_too).wait_recv()

    sums = [recv[i] for i in range(8)]
    for i in range(8, everyone):
        sums[i % 8] = sums[i % 8] + recv[i]
    while len(sums) > 1:
        sums = [a + b for a, b in zip(sums[0::2], sums[1::2])]
    out_ref[...] = sums[0]

    @pl.when(tm > 0)
    def _():
        halo.wait_send()

    for own_too in (0, 1):

        @pl.when(own == own_too)
        def _():
            all_of(everyone - own_too).wait_send()


def body(sizes, total, x_series, y_series):
    fwd, bwd = tables()
    zs, ys, xs = sizes
    pairs, length = x_series.shape
    blocks, extra = length // BLK, L // BLK
    f32, bf16 = jnp.float32, jnp.bfloat16
    dma = pltpu.SemaphoreType.DMA
    lagged = pl.pallas_call(
        functools.partial(kernel, sizes),
        out_shape=jax.ShapeDtypeStruct((1, L // xs), f32),
        in_specs=[pl.BlockSpec(memory_space=pl.ANY)] * 4,
        out_specs=pl.BlockSpec(memory_space=pltpu.VMEM),
        scratch_shapes=[
            pltpu.VMEM((pairs, length), f32),
            pltpu.VMEM((pairs, length), f32),
            pltpu.VMEM((pairs, L), f32),
            pltpu.VMEM((pairs, L), f32),
            pltpu.VMEM(fwd.shape, bf16),
            pltpu.VMEM(bwd.shape, bf16),
            pltpu.VMEM((blocks * pairs, 2 * BLK), bf16),
            pltpu.VMEM((blocks * pairs, N), f32),
            pltpu.VMEM(((blocks + extra) * pairs, N), f32),
            pltpu.VMEM((extra * pairs, N), f32),
            pltpu.VMEM((2 * extra * pairs, N), f32),
            pltpu.VMEM((pairs * xs, 1, L // xs), f32),
            pltpu.VMEM((2 * zs * ys, 1, L // xs), f32),
            dma((5,)),
            dma((2,)),
            dma,
            dma,
        ],
        compiler_params=pltpu.CompilerParams(collective_id=0, has_side_effects=True),
    )(x_series, y_series, jnp.asarray(fwd), jnp.asarray(bwd))
    return lagged * (1.0 / math.sqrt(total))


def solution(mesh):
    sizes = (8, 8, mesh.shape["pair"])
    total = 524288
    return jax.shard_map(
        functools.partial(body, sizes, total),
        mesh=mesh,
        in_specs=(P("pair", "tm"), P("pair", "tm")),
        out_specs=P("tm", "pair"),
        check_vma=False,
    )
```

```python
import functools
import math

import jax
import jax.numpy as jnp
import ml_dtypes
import numpy as np
from jax import lax
from jax.experimental import pallas as pl
from jax.experimental.pallas import tpu as pltpu
from jax.sharding import PartitionSpec as P

L = 512
BLK = 128
N = 2 * BLK
MESH = pl.DeviceIdType.MESH


def halves(array):
    high = array.astype(ml_dtypes.bfloat16)
    low = (array - high.astype(np.float64)).astype(ml_dtypes.bfloat16)
    return high, low


@functools.cache
def tables(total):
    theta = 2 * np.pi * (np.arange(BLK) + 0.5) / N
    turns = np.outer(np.arange(BLK), theta)
    high, low = halves(np.concatenate([np.cos(turns), np.sin(turns)], axis=1))
    forward = np.stack([np.concatenate([high, high]), np.concatenate([low, low])])
    high, low = halves(np.concatenate([np.cos(turns.T), -np.sin(turns.T)]) * (2.0 / N / math.sqrt(total)))
    return forward, np.concatenate([high, low], axis=1)


def high_low(value):
    high = value.astype(jnp.bfloat16)
    return high, (value - high.astype(jnp.float32)).astype(jnp.bfloat16)


def kernel(
    sizes, x_hbm, y_hbm, fwd_hbm, bwd_hbm, recv,
    xv, yv, lead, head, fwd, bwd, parts, fx, fy, res, rparts, send,
    load_sem, halo_sem, send_sem, recv_sem,
):
    zs, ys, xs = sizes
    pairs, length = xv.shape
    blocks, extra = length // BLK, L // BLK
    group = 2 * ys
    depth = zs // xs
    everyone = zs * group
    last = everyone - 1
    tm, mx = lax.axis_index("tm"), lax.axis_index("pair")
    mz, mg = tm // group, tm % group
    source_x = mz // depth
    own = jnp.where(source_x == mx, 1, 0)

    loads = [
        pltpu.make_async_copy(y_hbm.at[:, 0:L], lead, load_sem.at[0]),
        pltpu.make_async_copy(x_hbm, xv, load_sem.at[1]),
        pltpu.make_async_copy(fwd_hbm, fwd, load_sem.at[2]),
        pltpu.make_async_copy(y_hbm, yv, load_sem.at[3]),
        pltpu.make_async_copy(bwd_hbm, bwd, load_sem.at[4]),
    ]
    for load in loads:
        load.start()

    barrier = pltpu.get_barrier_semaphore()

    @pl.when(tm < last)
    def _():
        pl.semaphore_signal(barrier, inc=1, device_id=(tm + 1, mx), device_id_type=MESH)

    for step in range(1, everyone):
        other = lax.rem(tm + step, everyone)
        pl.semaphore_signal(barrier, inc=1, device_id=(other, source_x), device_id_type=MESH)

    @pl.when(own == 0)
    def _():
        pl.semaphore_signal(barrier, inc=1, device_id=(tm, source_x), device_id_type=MESH)

    def transform(value, at, into):
        count = value.shape[1] // BLK
        for j in range(count):
            high, low = high_low(value[:, j * BLK : (j + 1) * BLK])
            parts[j * pairs : (j + 1) * pairs, 0:BLK] = high
            parts[j * pairs : (j + 1) * pairs, BLK : 2 * BLK] = low
        rows = parts[0 : count * pairs, :]
        into[at * pairs : (at + count) * pairs, :] = jnp.dot(
            rows, fwd[0], preferred_element_type=jnp.float32
        ) + jnp.dot(rows, fwd[1], preferred_element_type=jnp.float32)

    loads[0].wait()
    pl.semaphore_wait(barrier, pairs * xs - own + jnp.where(tm > 0, 1, 0))
    halo = pltpu.make_async_remote_copy(
        src_ref=lead,
        dst_ref=head,
        send_sem=halo_sem.at[0],
        recv_sem=halo_sem.at[1],
        device_id=(jnp.maximum(tm - 1, 0), mx),
        device_id_type=MESH,
    )

    @pl.when(tm > 0)
    def _():
        halo.start()

    @pl.when(tm == last)
    def _():
        head[...] = jnp.zeros_like(head)

    loads[1].wait()
    loads[2].wait()
    transform(xv, 0, fx)

    loads[3].wait()
    transform(yv, 0, fy)

    lane = lax.broadcasted_iota(jnp.int32, (8, BLK), 1)
    sign = jnp.where(lane % 2 == 0, 1.0, -1.0).astype(jnp.float32)

    def take(ref, block, at):
        rows = pl.ds(pl.multiple_of(block * pairs + at, 8), 8)
        return ref[rows, 0:BLK], ref[rows, BLK : 2 * BLK]

    def products(at, first, past):
        sums = [None] * extra
        window = {}
        ahead = None
        for j in range(first, past):
            now = take(fy, j, at) if ahead is None else ahead
            ahead = take(fy, j + 1, at)
            window[j] = (now[0] - sign * ahead[1], now[1] + sign * ahead[0])
        terms = {}
        for q in range(extra):
            for b in range(blocks):
                if first <= b + q < past:
                    terms.setdefault(b, []).append(q)
        for b, lags in terms.items():
            cx, sx = take(fx, b, at)
            for q in lags:
                cz, sz = window[b + q]
                real, imag = cx * cz + sx * sz, sx * cz - cx * sz
                if sums[q] is not None:
                    real, imag = real + sums[q][0], imag + sums[q][1]
                sums[q] = (real, imag)
        return sums

    @pl.loop(0, pairs // 8)
    def _(g):
        at = pl.multiple_of(g * 8, 8)
        for q, (real, imag) in enumerate(products(at, 0, blocks - 1)):
            rows = pl.ds(pl.multiple_of(q * pairs + at, 8), 8)
            res[rows, 0:BLK] = real
            res[rows, BLK : 2 * BLK] = imag

    @pl.when(tm < last)
    def _():
        halo.wait_recv()

    transform(head, blocks, fy)
    for at in range(0, pairs, 8):
        for q, (real, imag) in enumerate(products(at, blocks - 1, blocks + extra - 1)):
            rows = slice(q * pairs + at, q * pairs + at + 8)
            for half, value in enumerate((real, imag)):
                columns = slice(half * BLK, (half + 1) * BLK)
                high, low = high_low(res[rows, columns] + value)
                rparts[rows, columns] = high.astype(jnp.float32)
                rparts[extra * pairs + q * pairs + at : extra * pairs + q * pairs + at + 8, columns] = low.astype(jnp.float32)

    loads[4].wait()
    both = jnp.dot(rparts[...].astype(jnp.bfloat16), bwd[...], preferred_element_type=jnp.float32)
    half = extra * pairs
    lagged = (both[0:half, 0:BLK] + both[0:half, BLK : 2 * BLK]) + (
        both[half:, 0:BLK] + both[half:, BLK : 2 * BLK]
    )
    send[...] = lagged.reshape(half, 1, BLK)

    def copy(row, q):
        return pltpu.make_async_remote_copy(
            src_ref=send.at[q * pairs + row],
            dst_ref=recv.at[tm],
            send_sem=send_sem,
            recv_sem=recv_sem,
            device_id=(mx * pairs + row, q),
            device_id_type=MESH,
        )

    order = [0]
    for d in range(1, ys // 2):
        order += [d, ys - d]
    order.append(ys // 2)
    for y in order:
        for e in range(depth):
            for c in (0, 1):
                row = e * group + y * 2 + c
                for step in range(1, xs):
                    copy(row, lax.rem(mx + step, xs)).start()

                @pl.when(mx * pairs + row != tm)
                def _():
                    copy(row, mx).start()

    kept = pltpu.make_async_copy(send.at[tm], recv.at[tm], load_sem.at[5])

    @pl.when(own == 1)
    def _():
        kept.start()

    def all_of(count):
        return pltpu.make_async_remote_copy(
            src_ref=send.at[pl.ds(0, count)],
            dst_ref=recv.at[pl.ds(0, count)],
            send_sem=send_sem,
            recv_sem=recv_sem,
            device_id=(tm, mx),
            device_id_type=MESH,
        )

    for own_too in (0, 1):

        @pl.when(own == own_too)
        def _():
            all_of(everyone - own_too).wait_recv()

    @pl.when(own == 1)
    def _():
        kept.wait()

    @pl.when(tm > 0)
    def _():
        halo.wait_send()

    for own_too in (0, 1):

        @pl.when(own == own_too)
        def _():
            all_of(everyone - own_too).wait_send()


def body(sizes, total, x_series, y_series):
    fwd, bwd = tables(total)
    zs, ys, xs = sizes
    pairs, length = x_series.shape
    blocks, extra = length // BLK, L // BLK
    f32, bf16 = jnp.float32, jnp.bfloat16
    dma = pltpu.SemaphoreType.DMA
    shares = pl.pallas_call(
        functools.partial(kernel, sizes),
        out_shape=pltpu.VMEM((2 * zs * ys, 1, L // xs), f32),
        in_specs=[pl.BlockSpec(memory_space=pl.ANY)] * 4,
        out_specs=pl.BlockSpec(memory_space=pl.ANY),
        scratch_shapes=[
            pltpu.VMEM((pairs, length), f32),
            pltpu.VMEM((pairs, length), f32),
            pltpu.VMEM((pairs, L), f32),
            pltpu.VMEM((pairs, L), f32),
            pltpu.VMEM(fwd.shape, bf16),
            pltpu.VMEM(bwd.shape, bf16),
            pltpu.VMEM((blocks * pairs, 2 * BLK), bf16),
            pltpu.VMEM((blocks * pairs, N), f32),
            pltpu.VMEM(((blocks + extra) * pairs, N), f32),
            pltpu.VMEM((extra * pairs, N), f32),
            pltpu.VMEM((2 * extra * pairs, N), f32),
            pltpu.VMEM((pairs * xs, 1, L // xs), f32),
            dma((6,)),
            dma((2,)),
            dma,
            dma,
        ],
        compiler_params=pltpu.CompilerParams(collective_id=0, has_side_effects=True),
    )(x_series, y_series, jnp.asarray(fwd), jnp.asarray(bwd))
    return jnp.sum(shares, axis=0)


def solution(mesh):
    sizes = (8, 8, mesh.shape["pair"])
    total = 524288
    return jax.shard_map(
        functools.partial(body, sizes, total),
        mesh=mesh,
        in_specs=(P("pair", "tm"), P("pair", "tm")),
        out_specs=P("tm", "pair"),
        check_vma=False,
    )
```

```python
import functools
import math

import jax
import jax.numpy as jnp
import ml_dtypes
import numpy as np
from jax import lax
from jax.experimental import pallas as pl
from jax.experimental.pallas import tpu as pltpu
from jax.sharding import PartitionSpec as P

L = 512
BLK = 128
N = 2 * BLK
MESH = pl.DeviceIdType.MESH


def halves(array):
    high = array.astype(ml_dtypes.bfloat16)
    low = (array - high.astype(np.float64)).astype(ml_dtypes.bfloat16)
    return high, low


@functools.cache
def tables(total):
    theta = 2 * np.pi * (np.arange(BLK) + 0.5) / N
    turns = np.outer(np.arange(BLK), theta)
    high, low = halves(np.concatenate([np.cos(turns), np.sin(turns)], axis=1))
    forward = np.stack([np.concatenate([high, high]), np.concatenate([low, low])])
    high, low = halves(np.concatenate([np.cos(turns.T), -np.sin(turns.T)]) * (2.0 / N / math.sqrt(total)))
    return forward, np.concatenate([high, low], axis=1)


def high_low(value):
    high = value.astype(jnp.bfloat16)
    return high, (value - high.astype(jnp.float32)).astype(jnp.bfloat16)


def kernel(
    sizes, x_hbm, y_hbm, fwd_hbm, bwd_hbm, recv,
    xv, yv, edges, halo, fwd, bwd, parts, fx, fy, fh, res, rparts, send,
    load_sem, halo_sem, send_sem, recv_sem,
):
    zs, ys, xs = sizes
    pairs, length = xv.shape
    blocks, extra = length // BLK, L // BLK
    near = extra // 2
    reach = near * BLK
    group = 2 * ys
    depth = zs // xs
    everyone = zs * group
    last = everyone - 1
    tm, mx = lax.axis_index("tm"), lax.axis_index("pair")
    mz, mg = tm // group, tm % group
    source_x = mz // depth
    own = jnp.where(source_x == mx, 1, 0)

    loads = [
        pltpu.make_async_copy(y_hbm.at[:, 0:reach], edges.at[0], load_sem.at[0]),
        pltpu.make_async_copy(x_hbm.at[:, length - reach : length], edges.at[1], load_sem.at[6]),
        pltpu.make_async_copy(x_hbm, xv, load_sem.at[1]),
        pltpu.make_async_copy(fwd_hbm, fwd, load_sem.at[2]),
        pltpu.make_async_copy(y_hbm, yv, load_sem.at[3]),
        pltpu.make_async_copy(bwd_hbm, bwd, load_sem.at[4]),
    ]
    for load in loads:
        load.start()

    barrier = pltpu.get_barrier_semaphore()

    for step, there in ((1, tm < last), (-1, tm > 0)):

        @pl.when(there)
        def _():
            pl.semaphore_signal(barrier, inc=1, device_id=(tm + step, mx), device_id_type=MESH)

    for other in range(everyone):

        @pl.when(jnp.logical_or(source_x != mx, tm != other))
        def _():
            pl.semaphore_signal(barrier, inc=1, device_id=(other, source_x), device_id_type=MESH)

    def transform(values, into):
        count = 0
        for value in values:
            for j in range(value.shape[1] // BLK):
                high, low = high_low(value[:, j * BLK : (j + 1) * BLK])
                parts[count * pairs : (count + 1) * pairs, 0:BLK] = high
                parts[count * pairs : (count + 1) * pairs, BLK : 2 * BLK] = low
                count += 1
        rows = parts[0 : count * pairs, :]
        into[...] = jnp.dot(rows, fwd[0], preferred_element_type=jnp.float32) + jnp.dot(
            rows, fwd[1], preferred_element_type=jnp.float32
        )

    loads[0].wait()
    loads[1].wait()
    neighbours = jnp.where(tm > 0, 1, 0) + jnp.where(tm < last, 1, 0)
    pl.semaphore_wait(barrier, pairs * xs - own + neighbours)

    def swap(side, other):
        return pltpu.make_async_remote_copy(
            src_ref=edges.at[side],
            dst_ref=halo.at[side],
            send_sem=halo_sem.at[side],
            recv_sem=halo_sem.at[2 + side],
            device_id=(other, mx),
            device_id_type=MESH,
        )

    to_before, to_next = swap(0, jnp.maximum(tm - 1, 0)), swap(1, jnp.minimum(tm + 1, last))

    @pl.when(tm > 0)
    def _():
        to_before.start()

    @pl.when(tm < last)
    def _():
        to_next.start()

    @pl.when(tm == last)
    def _():
        halo[0] = jnp.zeros((pairs, reach), jnp.float32)

    @pl.when(tm == 0)
    def _():
        halo[1] = jnp.zeros((pairs, reach), jnp.float32)

    loads[2].wait()
    loads[3].wait()
    transform([xv], fx)

    loads[4].wait()
    transform([yv], fy)

    lane = lax.broadcasted_iota(jnp.int32, (8, BLK), 1)
    sign = jnp.where(lane % 2 == 0, 1.0, -1.0).astype(jnp.float32)

    def take(ref, block, at):
        rows = pl.ds(pl.multiple_of(block * pairs + at, 8), 8)
        return ref[rows, 0:BLK], ref[rows, BLK : 2 * BLK]

    def turned(value):
        return -sign * value[1], sign * value[0]

    def plus(a, b):
        return b if a is None else (a[0] + b[0], a[1] + b[1])

    def add(sums, q, a, b):
        (ca, sa), (cb, sb) = a, b
        sums[q] = plus(sums[q], (ca * cb + sa * sb, sa * cb - ca * sb))

    def inner(at):
        window = {}
        now = take(fy, 0, at)
        for j in range(blocks - 1):
            ahead = take(fy, j + 1, at)
            window[j] = plus(now, turned(ahead))
            now = ahead
        sums = [None] * extra
        for b in range(blocks - 1):
            x = take(fx, b, at)
            for q in range(extra):
                if b + q < blocks - 1:
                    add(sums, q, x, window[b + q])
        return sums

    def outer(at):
        y = [take(fh, j, at) for j in range(near)]
        window = [plus(take(fy, blocks - 1, at), turned(y[0]))]
        window += [plus(y[j], turned(y[j + 1])) for j in range(near - 1)] + [y[near - 1]]
        sums = [None] * extra
        for b in range(blocks - extra, blocks):
            x = take(fx, b, at)
            for q in range(extra):
                if 0 <= b + q - (blocks - 1) <= near:
                    add(sums, q, x, window[b + q - (blocks - 1)])
        for b in range(near):
            x = take(fh, near + b, at)
            for q in range(extra):
                j = b - near + q
                if j >= near:
                    add(sums, q, x, plus(take(fy, j, at), turned(take(fy, j + 1, at))))
                elif j == near - 1:
                    add(sums, q, x, turned(take(fy, near, at)))
        return sums

    @pl.loop(0, pairs // 8)
    def _(g):
        at = pl.multiple_of(g * 8, 8)
        for q, (real, imag) in enumerate(inner(at)):
            rows = pl.ds(pl.multiple_of(q * pairs + at, 8), 8)
            res[rows, 0:BLK] = real
            res[rows, BLK : 2 * BLK] = imag

    @pl.when(tm < last)
    def _():
        to_before.wait_recv()

    @pl.when(tm > 0)
    def _():
        to_next.wait_recv()

    transform([halo.at[0], halo.at[1]], fh)
    for at in range(0, pairs, 8):
        for q, (real, imag) in enumerate(outer(at)):
            rows = slice(q * pairs + at, q * pairs + at + 8)
            for half, value in enumerate((real, imag)):
                columns = slice(half * BLK, (half + 1) * BLK)
                high, low = high_low(res[rows, columns] + value)
                rparts[rows, columns] = high.astype(jnp.float32)
                rparts[extra * pairs + q * pairs + at : extra * pairs + q * pairs + at + 8, columns] = low.astype(jnp.float32)

    loads[5].wait()
    both = jnp.dot(rparts[...].astype(jnp.bfloat16), bwd[...], preferred_element_type=jnp.float32)
    half = extra * pairs
    lagged = (both[0:half, 0:BLK] + both[0:half, BLK : 2 * BLK]) + (
        both[half:, 0:BLK] + both[half:, BLK : 2 * BLK]
    )
    send[...] = lagged.reshape(half, 1, BLK)

    def copy(row, q):
        return pltpu.make_async_remote_copy(
            src_ref=send.at[q * pairs + row],
            dst_ref=recv.at[tm],
            send_sem=send_sem,
            recv_sem=recv_sem,
            device_id=(mx * pairs + row, q),
            device_id_type=MESH,
        )

    own_at = jnp.where(own == 1, tm, -1)
    order = [0]
    for d in range(1, ys // 2):
        order += [d, ys - d]
    order.append(ys // 2)
    for y in order:
        for e in range(depth):
            for c in (0, 1):
                row = e * group + y * 2 + c
                for q in range(xs):

                    @pl.when(own_at != q * pairs + row)
                    def _():
                        copy(row, q).start()

    kept = pltpu.make_async_copy(send.at[tm], recv.at[tm], load_sem.at[5])

    @pl.when(own == 1)
    def _():
        kept.start()

    def all_of(count):
        return pltpu.make_async_remote_copy(
            src_ref=send.at[pl.ds(0, count)],
            dst_ref=recv.at[pl.ds(0, count)],
            send_sem=send_sem,
            recv_sem=recv_sem,
            device_id=(tm, mx),
            device_id_type=MESH,
        )

    for own_too in (0, 1):

        @pl.when(own == own_too)
        def _():
            all_of(everyone - own_too).wait_recv()

    @pl.when(own == 1)
    def _():
        kept.wait()

    @pl.when(tm > 0)
    def _():
        to_before.wait_send()

    @pl.when(tm < last)
    def _():
        to_next.wait_send()

    for own_too in (0, 1):

        @pl.when(own == own_too)
        def _():
            all_of(everyone - own_too).wait_send()


def body(sizes, total, x_series, y_series):
    fwd, bwd = tables(total)
    zs, ys, xs = sizes
    pairs, length = x_series.shape
    blocks, extra = length // BLK, L // BLK
    f32, bf16 = jnp.float32, jnp.bfloat16
    dma = pltpu.SemaphoreType.DMA
    shares = pl.pallas_call(
        functools.partial(kernel, sizes),
        out_shape=pltpu.VMEM((2 * zs * ys, 1, L // xs), f32),
        in_specs=[pl.BlockSpec(memory_space=pl.ANY)] * 4,
        out_specs=pl.BlockSpec(memory_space=pl.ANY),
        scratch_shapes=[
            pltpu.VMEM((pairs, length), f32),
            pltpu.VMEM((pairs, length), f32),
            pltpu.VMEM((2, pairs, L // 2), f32),
            pltpu.VMEM((2, pairs, L // 2), f32),
            pltpu.VMEM(fwd.shape, bf16),
            pltpu.VMEM(bwd.shape, bf16),
            pltpu.VMEM((blocks * pairs, 2 * BLK), bf16),
            pltpu.VMEM((blocks * pairs, N), f32),
            pltpu.VMEM((blocks * pairs, N), f32),
            pltpu.VMEM((extra * pairs, N), f32),
            pltpu.VMEM((extra * pairs, N), f32),
            pltpu.VMEM((2 * extra * pairs, N), f32),
            pltpu.VMEM((pairs * xs, 1, L // xs), f32),
            dma((7,)),
            dma((4,)),
            dma,
            dma,
        ],
        compiler_params=pltpu.CompilerParams(collective_id=0, has_side_effects=True),
    )(x_series, y_series, jnp.asarray(fwd), jnp.asarray(bwd))
    return jnp.sum(shares, axis=0)


def solution(mesh):
    sizes = (8, 8, mesh.shape["pair"])
    total = 524288
    return jax.shard_map(
        functools.partial(body, sizes, total),
        mesh=mesh,
        in_specs=(P("pair", "tm"), P("pair", "tm")),
        out_specs=P("tm", "pair"),
        check_vma=False,
    )
```

```python
import functools
import math

import jax
import jax.numpy as jnp
import ml_dtypes
import numpy as np
from jax import lax
from jax.experimental import pallas as pl
from jax.experimental.pallas import tpu as pltpu
from jax.sharding import PartitionSpec as P

L = 512
BLK = 128
N = 2 * BLK
MESH = pl.DeviceIdType.MESH


def halves(array):
    high = array.astype(ml_dtypes.bfloat16)
    low = (array - high.astype(np.float64)).astype(ml_dtypes.bfloat16)
    return high, low


@functools.cache
def tables(total):
    theta = 2 * np.pi * (np.arange(BLK) + 0.5) / N
    turns = np.outer(np.arange(BLK), theta)
    high, low = halves(np.concatenate([np.cos(turns), np.sin(turns)], axis=1))
    forward = np.stack([np.concatenate([high, high]), np.concatenate([low, low])])
    high, low = halves(np.concatenate([np.cos(turns.T), -np.sin(turns.T)]) * (2.0 / N / math.sqrt(total)))
    return forward, np.concatenate([high, low], axis=1)


def from_far(count):
    return sorted(range(1, count), key=lambda d: -min(d, count - d))


def high_low(value):
    high = value.astype(jnp.bfloat16)
    return high, (value - high.astype(jnp.float32)).astype(jnp.bfloat16)


def kernel(
    sizes, x_hbm, y_hbm, fwd_hbm, bwd_hbm, recv,
    xv, yv, edges, halo, fwd, bwd, parts, fx, fy, fh, res, rparts, send,
    load_sem, halo_sem, send_sem, recv_sem,
):
    zs, ys, xs = sizes
    pairs, length = xv.shape
    blocks, extra = length // BLK, L // BLK
    near = extra // 2
    reach = near * BLK
    group = 2 * ys
    depth = zs // xs
    everyone = zs * group
    last = everyone - 1
    tm, mx = lax.axis_index("tm"), lax.axis_index("pair")
    mz, mg = tm // group, tm % group
    source_x = mz // depth
    own = jnp.where(source_x == mx, 1, 0)

    loads = [
        pltpu.make_async_copy(y_hbm.at[:, 0:reach], edges.at[0], load_sem.at[0]),
        pltpu.make_async_copy(x_hbm.at[:, length - reach : length], edges.at[1], load_sem.at[6]),
        pltpu.make_async_copy(x_hbm, xv, load_sem.at[1]),
        pltpu.make_async_copy(fwd_hbm, fwd, load_sem.at[2]),
        pltpu.make_async_copy(y_hbm, yv, load_sem.at[3]),
        pltpu.make_async_copy(bwd_hbm, bwd, load_sem.at[4]),
    ]
    for load in loads:
        load.start()

    barrier = pltpu.get_barrier_semaphore()

    for step, there in ((1, tm < last), (-1, tm > 0)):

        @pl.when(there)
        def _():
            pl.semaphore_signal(barrier, inc=1, device_id=(tm + step, mx), device_id_type=MESH)

    def here(z, g):
        pl.semaphore_signal(
            barrier, inc=1, device_id=(z * group + g, source_x), device_id_type=MESH
        )

    for d in from_far(zs):
        z = lax.rem(mz + d, zs)
        for g in range(group):
            here(z, g)
    for d in range(1, group):
        here(mz, lax.rem(mg + d, group))

    @pl.when(own == 0)
    def _():
        here(mz, mg)

    def transform(values, into):
        count = 0
        for value in values:
            for j in range(value.shape[1] // BLK):
                high, low = high_low(value[:, j * BLK : (j + 1) * BLK])
                parts[count * pairs : (count + 1) * pairs, 0:BLK] = high
                parts[count * pairs : (count + 1) * pairs, BLK : 2 * BLK] = low
                count += 1
        rows = parts[0 : count * pairs, :]
        into[...] = jnp.dot(rows, fwd[0], preferred_element_type=jnp.float32) + jnp.dot(
            rows, fwd[1], preferred_element_type=jnp.float32
        )

    loads[0].wait()
    loads[1].wait()
    neighbours = jnp.where(tm > 0, 1, 0) + jnp.where(tm < last, 1, 0)
    pl.semaphore_wait(barrier, pairs * xs - own + neighbours)

    def swap(side, other):
        return pltpu.make_async_remote_copy(
            src_ref=edges.at[side],
            dst_ref=halo.at[side],
            send_sem=halo_sem.at[side],
            recv_sem=halo_sem.at[2 + side],
            device_id=(other, mx),
            device_id_type=MESH,
        )

    to_before, to_next = swap(0, jnp.maximum(tm - 1, 0)), swap(1, jnp.minimum(tm + 1, last))

    @pl.when(tm > 0)
    def _():
        to_before.start()

    @pl.when(tm < last)
    def _():
        to_next.start()

    @pl.when(tm == last)
    def _():
        halo[0] = jnp.zeros((pairs, reach), jnp.float32)

    @pl.when(tm == 0)
    def _():
        halo[1] = jnp.zeros((pairs, reach), jnp.float32)

    loads[2].wait()
    loads[3].wait()
    transform([xv], fx)

    loads[4].wait()
    transform([yv], fy)

    lane = lax.broadcasted_iota(jnp.int32, (8, BLK), 1)
    sign = jnp.where(lane % 2 == 0, 1.0, -1.0).astype(jnp.float32)

    def take(ref, block, at):
        rows = pl.ds(pl.multiple_of(block * pairs + at, 8), 8)
        return ref[rows, 0:BLK], ref[rows, BLK : 2 * BLK]

    def turned(value):
        return -sign * value[1], sign * value[0]

    def plus(a, b):
        return b if a is None else (a[0] + b[0], a[1] + b[1])

    def add(sums, q, a, b):
        (ca, sa), (cb, sb) = a, b
        sums[q] = plus(sums[q], (ca * cb + sa * sb, sa * cb - ca * sb))

    def inner(at):
        window = {}
        now = take(fy, 0, at)
        for j in range(blocks - 1):
            ahead = take(fy, j + 1, at)
            window[j] = plus(now, turned(ahead))
            now = ahead
        sums = [None] * extra
        for b in range(blocks - 1):
            x = take(fx, b, at)
            for q in range(extra):
                if b + q < blocks - 1:
                    add(sums, q, x, window[b + q])
        return sums

    def outer(at):
        y = [take(fh, j, at) for j in range(near)]
        window = [plus(take(fy, blocks - 1, at), turned(y[0]))]
        window += [plus(y[j], turned(y[j + 1])) for j in range(near - 1)] + [y[near - 1]]
        sums = [None] * extra
        for b in range(blocks - extra, blocks):
            x = take(fx, b, at)
            for q in range(extra):
                if 0 <= b + q - (blocks - 1) <= near:
                    add(sums, q, x, window[b + q - (blocks - 1)])
        for b in range(near):
            x = take(fh, near + b, at)
            for q in range(extra):
                j = b - near + q
                if j >= near:
                    add(sums, q, x, plus(take(fy, j, at), turned(take(fy, j + 1, at))))
                elif j == near - 1:
                    add(sums, q, x, turned(take(fy, near, at)))
        return sums

    @pl.loop(0, pairs // 8)
    def _(g):
        at = pl.multiple_of(g * 8, 8)
        for q, (real, imag) in enumerate(inner(at)):
            rows = pl.ds(pl.multiple_of(q * pairs + at, 8), 8)
            res[rows, 0:BLK] = real
            res[rows, BLK : 2 * BLK] = imag

    @pl.when(tm < last)
    def _():
        to_before.wait_recv()

    @pl.when(tm > 0)
    def _():
        to_next.wait_recv()

    transform([halo.at[0], halo.at[1]], fh)
    for at in range(0, pairs, 8):
        for q, (real, imag) in enumerate(outer(at)):
            rows = slice(q * pairs + at, q * pairs + at + 8)
            for half, value in enumerate((real, imag)):
                columns = slice(half * BLK, (half + 1) * BLK)
                high, low = high_low(res[rows, columns] + value)
                rparts[rows, columns] = high.astype(jnp.float32)
                rparts[extra * pairs + q * pairs + at : extra * pairs + q * pairs + at + 8, columns] = low.astype(jnp.float32)

    loads[5].wait()
    both = jnp.dot(rparts[...].astype(jnp.bfloat16), bwd[...], preferred_element_type=jnp.float32)
    half = extra * pairs
    lagged = (both[0:half, 0:BLK] + both[0:half, BLK : 2 * BLK]) + (
        both[half:, 0:BLK] + both[half:, BLK : 2 * BLK]
    )
    send[...] = lagged.reshape(half, 1, BLK)

    def copy(row, q):
        return pltpu.make_async_remote_copy(
            src_ref=send.at[q * pairs + row],
            dst_ref=recv.at[tm],
            send_sem=send_sem,
            recv_sem=recv_sem,
            device_id=(mx * pairs + row, q),
            device_id_type=MESH,
        )

    own_at = jnp.where(own == 1, tm, -1)
    for e in range(depth):
        for y in range(ys):
            for c in (1, 0):
                row = e * group + y * 2 + c
                for q in range(xs):

                    @pl.when(own_at != q * pairs + row)
                    def _():
                        copy(row, q).start()

    kept = pltpu.make_async_copy(send.at[tm], recv.at[tm], load_sem.at[5])

    @pl.when(own == 1)
    def _():
        kept.start()

    def all_of(count):
        return pltpu.make_async_remote_copy(
            src_ref=send.at[pl.ds(0, count)],
            dst_ref=recv.at[pl.ds(0, count)],
            send_sem=send_sem,
            recv_sem=recv_sem,
            device_id=(tm, mx),
            device_id_type=MESH,
        )

    for own_too in (0, 1):

        @pl.when(own == own_too)
        def _():
            all_of(everyone - own_too).wait_recv()

    @pl.when(own == 1)
    def _():
        kept.wait()

    @pl.when(tm > 0)
    def _():
        to_before.wait_send()

    @pl.when(tm < last)
    def _():
        to_next.wait_send()

    for own_too in (0, 1):

        @pl.when(own == own_too)
        def _():
            all_of(everyone - own_too).wait_send()


def body(sizes, total, x_series, y_series):
    fwd, bwd = tables(total)
    zs, ys, xs = sizes
    pairs, length = x_series.shape
    blocks, extra = length // BLK, L // BLK
    f32, bf16 = jnp.float32, jnp.bfloat16
    dma = pltpu.SemaphoreType.DMA
    shares = pl.pallas_call(
        functools.partial(kernel, sizes),
        out_shape=pltpu.VMEM((2 * zs * ys, 1, L // xs), f32),
        in_specs=[pl.BlockSpec(memory_space=pl.ANY)] * 4,
        out_specs=pl.BlockSpec(memory_space=pl.ANY),
        scratch_shapes=[
            pltpu.VMEM((pairs, length), f32),
            pltpu.VMEM((pairs, length), f32),
            pltpu.VMEM((2, pairs, L // 2), f32),
            pltpu.VMEM((2, pairs, L // 2), f32),
            pltpu.VMEM(fwd.shape, bf16),
            pltpu.VMEM(bwd.shape, bf16),
            pltpu.VMEM((blocks * pairs, 2 * BLK), bf16),
            pltpu.VMEM((blocks * pairs, N), f32),
            pltpu.VMEM((blocks * pairs, N), f32),
            pltpu.VMEM((extra * pairs, N), f32),
            pltpu.VMEM((extra * pairs, N), f32),
            pltpu.VMEM((2 * extra * pairs, N), f32),
            pltpu.VMEM((pairs * xs, 1, L // xs), f32),
            dma((7,)),
            dma((4,)),
            dma,
            dma,
        ],
        compiler_params=pltpu.CompilerParams(collective_id=0, has_side_effects=True),
    )(x_series, y_series, jnp.asarray(fwd), jnp.asarray(bwd))
    return jnp.sum(shares, axis=0)


def solution(mesh):
    sizes = (8, 8, mesh.shape["pair"])
    total = 524288
    return jax.shard_map(
        functools.partial(body, sizes, total),
        mesh=mesh,
        in_specs=(P("pair", "tm"), P("pair", "tm")),
        out_specs=P("tm", "pair"),
        check_vma=False,
    )
```

```python
import functools
import math

import jax
import jax.numpy as jnp
import ml_dtypes
import numpy as np
from jax import lax
from jax.experimental import pallas as pl
from jax.experimental.pallas import tpu as pltpu
from jax.sharding import PartitionSpec as P

L = 512
BLK = 128
N = 2 * BLK
MESH = pl.DeviceIdType.MESH


def halves(array):
    high = array.astype(ml_dtypes.bfloat16)
    low = (array - high.astype(np.float64)).astype(ml_dtypes.bfloat16)
    return high, low


@functools.cache
def tables(total):
    theta = 2 * np.pi * (np.arange(BLK) + 0.5) / N
    turns = np.outer(np.arange(BLK), theta)
    high, low = halves(np.concatenate([np.cos(turns), np.sin(turns)], axis=1))
    forward = np.stack([np.concatenate([high, high]), np.concatenate([low, low])])
    high, low = halves(np.concatenate([np.cos(turns.T), -np.sin(turns.T)]) * (2.0 / N / math.sqrt(total)))
    return forward, np.concatenate([high, low], axis=1)


def from_far(count):
    return sorted(range(1, count), key=lambda d: -min(d, count - d))


def high_low(value):
    high = value.astype(jnp.bfloat16)
    return high, (value - high.astype(jnp.float32)).astype(jnp.bfloat16)


def kernel(
    sizes, x_hbm, y_hbm, fwd_hbm, bwd_hbm, recv,
    xv, yv, edges, halo, fwd, bwd,
    px0, px1, py0, py1, ph0, ph1, fx0, fx1, fy0, fy1, fh0, fh1, res, rparts, send,
    load_sem, halo_sem, send_sem, recv_sem, told,
):
    zs, ys, xs = sizes
    pairs, length = xv.shape
    blocks, extra = length // BLK, L // BLK
    near = extra // 2
    reach = near * BLK
    half = pairs // 2
    first, second = slice(0, half), slice(half, pairs)
    group = 2 * ys
    depth = zs // xs
    everyone = zs * group
    last = everyone - 1
    tm, mx = lax.axis_index("tm"), lax.axis_index("pair")
    mz, mg = tm // group, tm % group
    my, mc = mg // 2, mg % 2
    source_x = mz // depth
    own = jnp.where(source_x == mx, 1, 0)

    loads = [
        pltpu.make_async_copy(y_hbm.at[:, 0:reach], edges.at[0], load_sem.at[0]),
        pltpu.make_async_copy(x_hbm.at[:, length - reach : length], edges.at[1], load_sem.at[6]),
        pltpu.make_async_copy(x_hbm, xv, load_sem.at[1]),
        pltpu.make_async_copy(fwd_hbm, fwd, load_sem.at[2]),
        pltpu.make_async_copy(y_hbm, yv, load_sem.at[3]),
        pltpu.make_async_copy(bwd_hbm, bwd, load_sem.at[4]),
    ]
    for load in loads:
        load.start()

    barrier = pltpu.get_barrier_semaphore()

    def arrived(device, x):
        pl.semaphore_signal(barrier, inc=1, device_id=(device, x), device_id_type=MESH)

    def tell(which, device):
        pl.semaphore_signal(told.at[which], inc=1, device_id=(device, mx), device_id_type=MESH)

    @pl.when(mc == 1)
    def _():
        arrived(tm - 1, mx)

    @pl.when(jnp.logical_and(mc == 1, tm < last))
    def _():
        arrived(tm + 1, mx)

    def greet():
        for d in from_far(zs):
            z = lax.rem(mz + d, zs)
            for y in range(ys):
                arrived(z * group + 2 * y + 1, source_x)
        for d in range(1, ys):
            arrived(mz * group + 2 * lax.rem(my + d, ys) + 1, source_x)

        @pl.when(jnp.logical_or(own == 0, mc == 0))
        def _():
            arrived(mz * group + 2 * my + 1, source_x)

    def transform(values, part, into):
        count = 0
        for value in values:
            for j in range(value.shape[1] // BLK):
                high, low = high_low(value[:, j * BLK : (j + 1) * BLK])
                part[count * half : (count + 1) * half, 0:BLK] = high
                part[count * half : (count + 1) * half, BLK : 2 * BLK] = low
                count += 1
        rows = part[0 : count * half, :]
        into[...] = jnp.dot(rows, fwd[0], preferred_element_type=jnp.float32) + jnp.dot(
            rows, fwd[1], preferred_element_type=jnp.float32
        )

    def swap(side, other):
        return pltpu.make_async_remote_copy(
            src_ref=edges.at[side],
            dst_ref=halo.at[side],
            send_sem=halo_sem.at[side],
            recv_sem=halo_sem.at[2 + side],
            device_id=(other, mx),
            device_id_type=MESH,
        )

    to_before, to_next = swap(0, jnp.maximum(tm - 1, 0)), swap(1, jnp.minimum(tm + 1, last))

    @pl.when(mc == 0)
    def _():
        pl.semaphore_wait(barrier, 1 + jnp.where(tm > 0, 1, 0))
        tell(0, tm + 1)

    @pl.when(jnp.logical_and(mc == 0, tm > 0))
    def _():
        tell(1, tm - 1)

    @pl.when(mc == 1)
    def _():
        greet()
        pl.semaphore_wait(told.at[0], 1)

    loads[0].wait()

    @pl.when(tm > 0)
    def _():
        to_before.start()

    @pl.when(mc == 0)
    def _():
        greet()

    loads[1].wait()

    @pl.when(tm == last)
    def _():
        halo[0] = jnp.zeros((pairs, reach), jnp.float32)

    @pl.when(tm == 0)
    def _():
        halo[1] = jnp.zeros((pairs, reach), jnp.float32)

    lane = lax.broadcasted_iota(jnp.int32, (8, BLK), 1)
    sign = jnp.where(lane % 2 == 0, 1.0, -1.0).astype(jnp.float32)

    def take(ref, block, at):
        return (
            ref[block * half + at : block * half + at + 8, 0:BLK],
            ref[block * half + at : block * half + at + 8, BLK : 2 * BLK],
        )

    def turned(value):
        return -sign * value[1], sign * value[0]

    def plus(a, b):
        return b if a is None else (a[0] + b[0], a[1] + b[1])

    def left(x):
        return x[0], x[0] - x[1], x[0] + x[1]

    def right(z):
        return z[0] + z[1], z[1], z[0]

    def add(sums, q, x, z):
        new = [u * v for u, v in zip(x, z)]
        sums[q] = new if sums[q] is None else [u + v for u, v in zip(sums[q], new)]

    def complex_of(sums):
        return [(a - b, c - a) for a, b, c in sums]

    def inner(xs_, ys_, at):
        sums = [None] * extra
        window = {}
        now = take(ys_, 0, at)
        for j in range(blocks - 1):
            ahead = take(ys_, j + 1, at)
            z = right(plus(now, turned(ahead)))
            now = ahead
            window[j] = left(take(xs_, j, at))
            for q in range(min(extra, j + 1)):
                add(sums, q, window[j - q], z)
        return complex_of(sums)

    def outer(xs_, ys_, hs_, at):
        y = [take(hs_, j, at) for j in range(near)]
        window = [plus(take(ys_, blocks - 1, at), turned(y[0]))]
        window += [plus(y[j], turned(y[j + 1])) for j in range(near - 1)] + [y[near - 1]]
        window = [right(z) for z in window]
        sums = [None] * extra
        for b in range(blocks - extra, blocks):
            x = left(take(xs_, b, at))
            for q in range(extra):
                if 0 <= b + q - (blocks - 1) <= near:
                    add(sums, q, x, window[b + q - (blocks - 1)])
        for b in range(near):
            x = left(take(hs_, near + b, at))
            for q in range(extra):
                j = b - near + q
                if j >= near:
                    add(sums, q, x, right(plus(take(ys_, j, at), turned(take(ys_, j + 1, at)))))
                elif j == near - 1:
                    add(sums, q, x, right(turned(take(ys_, near, at))))
        return complex_of(sums)

    def inner_products(xs_, ys_, base):
        for at in range(0, half, 8):
            for q, (real, imag) in enumerate(inner(xs_, ys_, at)):
                rows = slice(q * pairs + base + at, q * pairs + base + at + 8)
                res[rows, 0:BLK] = real
                res[rows, BLK : 2 * BLK] = imag

    loads[2].wait()
    loads[3].wait()
    transform([xv.at[first]], px0, fx0)

    @pl.when(jnp.logical_and(mc == 1, tm < last))
    def _():
        pl.semaphore_wait(told.at[1], 1)

    @pl.when(tm < last)
    def _():
        to_next.start()

    loads[4].wait()
    loads[5].wait()
    transform([yv.at[first]], py0, fy0)
    transform([xv.at[second]], px1, fx1)
    inner_products(fx0, fy0, 0)
    transform([yv.at[second]], py1, fy1)
    inner_products(fx1, fy1, half)

    @pl.when(mc == 1)
    def _():
        pl.semaphore_wait(barrier, pairs * xs - own)
        tell(2, tm - 1)

    @pl.when(tm < last)
    def _():
        to_before.wait_recv()

    @pl.when(tm > 0)
    def _():
        to_next.wait_recv()

    transform([halo.at[0, first], halo.at[1, first]], ph0, fh0)
    transform([halo.at[0, second], halo.at[1, second]], ph1, fh1)
    for base, sources in ((0, (fx0, fy0, fh0)), (half, (fx1, fy1, fh1))):
        for at in range(0, half, 8):
            for q, values in enumerate(outer(*sources, at)):
                rows = slice(q * pairs + base + at, q * pairs + base + at + 8)
                under = slice(pairs * extra + rows.start, pairs * extra + rows.stop)
                for part, value in enumerate(values):
                    columns = slice(part * BLK, (part + 1) * BLK)
                    rparts[rows, columns], rparts[under, columns] = high_low(res[rows, columns] + value)

    both = jnp.dot(rparts[...], bwd[...], preferred_element_type=jnp.float32)
    middle = extra * pairs
    lagged = (both[0:middle, 0:BLK] + both[0:middle, BLK : 2 * BLK]) + (
        both[middle:, 0:BLK] + both[middle:, BLK : 2 * BLK]
    )
    send[...] = lagged.reshape(middle, 1, BLK)

    @pl.when(mc == 0)
    def _():
        pl.semaphore_wait(told.at[2], 1)

    def copy(row, q):
        return pltpu.make_async_remote_copy(
            src_ref=send.at[q * pairs + row],
            dst_ref=recv.at[tm],
            send_sem=send_sem,
            recv_sem=recv_sem,
            device_id=(mx * pairs + row, q),
            device_id_type=MESH,
        )

    own_at = jnp.where(own == 1, tm, -1)
    for e in range(depth):
        for y in range(ys):
            for c in (1, 0):
                row = e * group + y * 2 + c
                for q in range(xs):

                    @pl.when(own_at != q * pairs + row)
                    def _():
                        copy(row, q).start()

    kept = pltpu.make_async_copy(send.at[tm], recv.at[tm], load_sem.at[5])

    @pl.when(own == 1)
    def _():
        kept.start()

    def all_of(count):
        return pltpu.make_async_remote_copy(
            src_ref=send.at[pl.ds(0, count)],
            dst_ref=recv.at[pl.ds(0, count)],
            send_sem=send_sem,
            recv_sem=recv_sem,
            device_id=(tm, mx),
            device_id_type=MESH,
        )

    for own_too in (0, 1):

        @pl.when(own == own_too)
        def _():
            all_of(everyone - own_too).wait_recv()

    @pl.when(own == 1)
    def _():
        kept.wait()

    @pl.when(tm > 0)
    def _():
        to_before.wait_send()

    @pl.when(tm < last)
    def _():
        to_next.wait_send()

    for own_too in (0, 1):

        @pl.when(own == own_too)
        def _():
            all_of(everyone - own_too).wait_send()


def body(sizes, total, x_series, y_series):
    fwd, bwd = tables(total)
    zs, ys, xs = sizes
    pairs, length = x_series.shape
    blocks, extra = length // BLK, L // BLK
    f32, bf16 = jnp.float32, jnp.bfloat16
    dma = pltpu.SemaphoreType.DMA
    shares = pl.pallas_call(
        functools.partial(kernel, sizes),
        out_shape=pltpu.VMEM((2 * zs * ys, 1, L // xs), f32),
        in_specs=[pl.BlockSpec(memory_space=pl.ANY)] * 4,
        out_specs=pl.BlockSpec(memory_space=pl.ANY),
        scratch_shapes=[
            pltpu.VMEM((pairs, length), f32),
            pltpu.VMEM((pairs, length), f32),
            pltpu.VMEM((2, pairs, L // 2), f32),
            pltpu.VMEM((2, pairs, L // 2), f32),
            pltpu.VMEM(fwd.shape, bf16),
            pltpu.VMEM(bwd.shape, bf16),
            *[pltpu.VMEM((blocks * pairs // 2, 2 * BLK), bf16)] * 4,
            *[pltpu.VMEM((extra * pairs // 2, 2 * BLK), bf16)] * 2,
            *[pltpu.VMEM((blocks * pairs // 2, N), f32)] * 4,
            *[pltpu.VMEM((extra * pairs // 2, N), f32)] * 2,
            pltpu.VMEM((extra * pairs, N), f32),
            pltpu.VMEM((2 * extra * pairs, N), bf16),
            pltpu.VMEM((pairs * xs, 1, L // xs), f32),
            dma((7,)),
            dma((4,)),
            dma,
            dma,
            pltpu.SemaphoreType.REGULAR((3,)),
        ],
        compiler_params=pltpu.CompilerParams(collective_id=0, has_side_effects=True),
    )(x_series, y_series, jnp.asarray(fwd), jnp.asarray(bwd))
    return jnp.sum(shares, axis=0)


def solution(mesh):
    sizes = (8, 8, mesh.shape["pair"])
    total = 524288
    return jax.shard_map(
        functools.partial(body, sizes, total),
        mesh=mesh,
        in_specs=(P("pair", "tm"), P("pair", "tm")),
        out_specs=P("tm", "pair"),
        check_vma=False,
    )
```

```python
import functools
import math

import jax
import jax.numpy as jnp
import ml_dtypes
import numpy as np
from jax import lax
from jax.experimental import pallas as pl
from jax.experimental.pallas import tpu as pltpu
from jax.sharding import PartitionSpec as P

L = 512
BLK = 128
N = 2 * BLK
MESH = pl.DeviceIdType.MESH


def halves(array):
    high = array.astype(ml_dtypes.bfloat16)
    low = (array - high.astype(np.float64)).astype(ml_dtypes.bfloat16)
    return high, low


@functools.cache
def tables(total):
    theta = 2 * np.pi * (np.arange(BLK) + 0.5) / N
    turns = np.outer(np.arange(BLK), theta)
    high, low = halves(np.concatenate([np.cos(turns), np.sin(turns)], axis=1))
    forward = np.stack([np.concatenate([high, high]), np.concatenate([low, low])])
    high, low = halves(np.concatenate([np.cos(turns.T), -np.sin(turns.T)]) * (2.0 / N / math.sqrt(total)))
    return forward, np.concatenate([high, low], axis=1)


def from_far(count):
    return sorted(range(1, count), key=lambda d: -min(d, count - d))


def high_low(value):
    high = value.astype(jnp.bfloat16)
    return high, (value - high.astype(jnp.float32)).astype(jnp.bfloat16)


def kernel(
    sizes, x_hbm, y_hbm, fwd_hbm, bwd_hbm, recv,
    xv, yv, lead, head, fwd, bwd,
    px0, px1, py0, py1, ph0, ph1, fx0, fx1, fy0, fy1, fh0, fh1, res0, res1, split0, split1, send,
    load_sem, halo_sem, send_sem, recv_sem, told,
):
    zs, ys, xs = sizes
    pairs, length = xv.shape
    blocks, extra = length // BLK, L // BLK
    half = pairs // 2
    first, second = slice(0, half), slice(half, pairs)
    group = 2 * ys
    depth = zs // xs
    everyone = zs * group
    last = everyone - 1
    tm, mx = lax.axis_index("tm"), lax.axis_index("pair")
    mz, mg = tm // group, tm % group
    my, mc = mg // 2, mg % 2
    source_x = mz // depth
    own = jnp.where(source_x == mx, 1, 0)

    loads = [
        pltpu.make_async_copy(y_hbm.at[:, 0:L], lead, load_sem.at[0]),
        pltpu.make_async_copy(x_hbm, xv, load_sem.at[1]),
        pltpu.make_async_copy(fwd_hbm, fwd, load_sem.at[2]),
        pltpu.make_async_copy(y_hbm, yv, load_sem.at[3]),
        pltpu.make_async_copy(bwd_hbm, bwd, load_sem.at[4]),
    ]
    for load in loads:
        load.start()

    barrier = pltpu.get_barrier_semaphore()

    def arrived(device, x):
        pl.semaphore_signal(barrier, inc=1, device_id=(device, x), device_id_type=MESH)

    def tell(which, device):
        pl.semaphore_signal(told.at[which], inc=1, device_id=(device, mx), device_id_type=MESH)

    @pl.when(mc == 1)
    def _():
        arrived(tm - 1, mx)

    @pl.when(jnp.logical_and(mc == 1, tm < last))
    def _():
        arrived(tm + 1, mx)

    def greet():
        for d in from_far(zs):
            z = lax.rem(mz + d, zs)
            for y in range(ys):
                arrived(z * group + 2 * y + 1, source_x)
        for d in range(1, ys):
            arrived(mz * group + 2 * lax.rem(my + d, ys) + 1, source_x)

        @pl.when(jnp.logical_or(own == 0, mc == 0))
        def _():
            arrived(mz * group + 2 * my + 1, source_x)

    def transform(values, part, into):
        count = 0
        for value in values:
            for j in range(value.shape[1] // BLK):
                high, low = high_low(value[:, j * BLK : (j + 1) * BLK])
                part[count * half : (count + 1) * half, 0:BLK] = high
                part[count * half : (count + 1) * half, BLK : 2 * BLK] = low
                count += 1
        rows = part[0 : count * half, :]
        into[...] = jnp.dot(rows, fwd[0], preferred_element_type=jnp.float32) + jnp.dot(
            rows, fwd[1], preferred_element_type=jnp.float32
        )

    to_before = pltpu.make_async_remote_copy(
        src_ref=lead,
        dst_ref=head,
        send_sem=halo_sem.at[0],
        recv_sem=halo_sem.at[1],
        device_id=(jnp.maximum(tm - 1, 0), mx),
        device_id_type=MESH,
    )

    @pl.when(mc == 0)
    def _():
        pl.semaphore_wait(barrier, 1 + jnp.where(tm > 0, 1, 0))
        tell(0, tm + 1)

    @pl.when(mc == 1)
    def _():
        greet()
        pl.semaphore_wait(told.at[0], 1)

    loads[0].wait()

    @pl.when(tm > 0)
    def _():
        to_before.start()

    @pl.when(mc == 0)
    def _():
        greet()

    @pl.when(tm == last)
    def _():
        head[...] = jnp.zeros_like(head)

    lane = lax.broadcasted_iota(jnp.int32, (8, BLK), 1)
    sign = jnp.where(lane % 2 == 0, 1.0, -1.0).astype(jnp.float32)

    def take(ref, block, at):
        return (
            ref[block * half + at : block * half + at + 8, 0:BLK],
            ref[block * half + at : block * half + at + 8, BLK : 2 * BLK],
        )

    def turned(value):
        return -sign * value[1], sign * value[0]

    def plus(a, b):
        return b if a is None else (a[0] + b[0], a[1] + b[1])

    def left(x):
        return x[0], x[0] - x[1], x[0] + x[1]

    def right(z):
        return z[0] + z[1], z[1], z[0]

    def add(sums, q, x, z):
        new = [u * v for u, v in zip(x, z)]
        sums[q] = new if sums[q] is None else [u + v for u, v in zip(sums[q], new)]

    def complex_of(sums):
        return [(a - b, c - a) for a, b, c in sums]

    def inner(xs_, ys_, at):
        sums = [None] * extra
        window = {}
        now = take(ys_, 0, at)
        for j in range(blocks - 1):
            ahead = take(ys_, j + 1, at)
            z = right(plus(now, turned(ahead)))
            now = ahead
            window[j] = left(take(xs_, j, at))
            for q in range(min(extra, j + 1)):
                add(sums, q, window[j - q], z)
        return complex_of(sums)

    def outer(xs_, ys_, hs_, at):
        y = [take(ys_, blocks - 1, at)] + [take(hs_, j, at) for j in range(extra)]
        window = [right(plus(y[j], turned(y[j + 1]))) for j in range(extra)]
        sums = [None] * extra
        for b in range(blocks - extra, blocks):
            x = left(take(xs_, b, at))
            for q in range(extra):
                if b + q >= blocks - 1:
                    add(sums, q, x, window[b + q - (blocks - 1)])
        return complex_of(sums)

    def inner_products(xs_, ys_, into):
        for at in range(0, half, 8):
            for q, (real, imag) in enumerate(inner(xs_, ys_, at)):
                rows = slice(q * half + at, q * half + at + 8)
                into[rows, 0:BLK] = real
                into[rows, BLK : 2 * BLK] = imag

    loads[1].wait()
    loads[2].wait()
    transform([xv.at[first]], px0, fx0)

    loads[3].wait()
    loads[4].wait()
    transform([yv.at[first]], py0, fy0)
    transform([xv.at[second]], px1, fx1)
    inner_products(fx0, fy0, res0)
    transform([yv.at[second]], py1, fy1)
    inner_products(fx1, fy1, res1)

    @pl.when(mc == 1)
    def _():
        pl.semaphore_wait(barrier, pairs * xs - own)
        tell(1, tm - 1)

    @pl.when(tm < last)
    def _():
        to_before.wait_recv()

    def finish(base, xs_, ys_, edge, part, hs_, sums, split):
        transform(edge, part, hs_)
        middle = extra * half
        for at in range(0, half, 8):
            for q, values in enumerate(outer(xs_, ys_, hs_, at)):
                rows = slice(q * half + at, q * half + at + 8)
                under = slice(middle + rows.start, middle + rows.stop)
                for which, value in enumerate(values):
                    columns = slice(which * BLK, (which + 1) * BLK)
                    split[rows, columns], split[under, columns] = high_low(
                        sums[rows, columns] + value
                    )
        both = jnp.dot(split[...], bwd[...], preferred_element_type=jnp.float32)
        lagged = (both[0:middle, 0:BLK] + both[0:middle, BLK : 2 * BLK]) + (
            both[middle:, 0:BLK] + both[middle:, BLK : 2 * BLK]
        )
        for q in range(extra):
            send[q * pairs + base : q * pairs + base + half] = lagged[
                q * half : (q + 1) * half
            ].reshape(half, 1, BLK)

    def copy(row, q):
        return pltpu.make_async_remote_copy(
            src_ref=send.at[q * pairs + row],
            dst_ref=recv.at[tm],
            send_sem=send_sem,
            recv_sem=recv_sem,
            device_id=(mx * pairs + row, q),
            device_id_type=MESH,
        )

    own_at = jnp.where(own == 1, tm, -1)
    def send_rows(rows):
        for y in range(ys):
            for row in rows:
                if row // 2 % ys == y:
                    for q in range(xs):

                        @pl.when(own_at != q * pairs + row)
                        def _():
                            copy(row, q).start()

    finish(0, fx0, fy0, [head.at[first]], ph0, fh0, res0, split0)

    @pl.when(mc == 0)
    def _():
        pl.semaphore_wait(told.at[1], 1)

    send_rows(range(half - 1, -1, -1))
    finish(half, fx1, fy1, [head.at[second]], ph1, fh1, res1, split1)
    send_rows(range(pairs - 1, half - 1, -1))

    kept = pltpu.make_async_copy(send.at[tm], recv.at[tm], load_sem.at[5])

    @pl.when(own == 1)
    def _():
        kept.start()

    def all_of(count):
        return pltpu.make_async_remote_copy(
            src_ref=send.at[pl.ds(0, count)],
            dst_ref=recv.at[pl.ds(0, count)],
            send_sem=send_sem,
            recv_sem=recv_sem,
            device_id=(tm, mx),
            device_id_type=MESH,
        )

    for own_too in (0, 1):

        @pl.when(own == own_too)
        def _():
            all_of(everyone - own_too).wait_recv()

    @pl.when(own == 1)
    def _():
        kept.wait()

    @pl.when(tm > 0)
    def _():
        to_before.wait_send()

    for own_too in (0, 1):

        @pl.when(own == own_too)
        def _():
            all_of(everyone - own_too).wait_send()


def body(sizes, total, x_series, y_series):
    fwd, bwd = tables(total)
    zs, ys, xs = sizes
    pairs, length = x_series.shape
    blocks, extra = length // BLK, L // BLK
    f32, bf16 = jnp.float32, jnp.bfloat16
    dma = pltpu.SemaphoreType.DMA
    shares = pl.pallas_call(
        functools.partial(kernel, sizes),
        out_shape=pltpu.VMEM((2 * zs * ys, 1, L // xs), f32),
        in_specs=[pl.BlockSpec(memory_space=pl.ANY)] * 4,
        out_specs=pl.BlockSpec(memory_space=pl.ANY),
        scratch_shapes=[
            pltpu.VMEM((pairs, length), f32),
            pltpu.VMEM((pairs, length), f32),
            pltpu.VMEM((pairs, L), f32),
            pltpu.VMEM((pairs, L), f32),
            pltpu.VMEM(fwd.shape, bf16),
            pltpu.VMEM(bwd.shape, bf16),
            *[pltpu.VMEM((blocks * pairs // 2, 2 * BLK), bf16)] * 4,
            *[pltpu.VMEM((extra * pairs // 2, 2 * BLK), bf16)] * 2,
            *[pltpu.VMEM((blocks * pairs // 2, N), f32)] * 4,
            *[pltpu.VMEM((extra * pairs // 2, N), f32)] * 2,
            *[pltpu.VMEM((extra * pairs // 2, N), f32)] * 2,
            *[pltpu.VMEM((extra * pairs, N), bf16)] * 2,
            pltpu.VMEM((pairs * xs, 1, L // xs), f32),
            dma((6,)),
            dma((2,)),
            dma,
            dma,
            pltpu.SemaphoreType.REGULAR((2,)),
        ],
        compiler_params=pltpu.CompilerParams(collective_id=0, has_side_effects=True),
    )(x_series, y_series, jnp.asarray(fwd), jnp.asarray(bwd))
    return jnp.sum(shares, axis=0)


def solution(mesh):
    sizes = (8, 8, mesh.shape["pair"])
    total = 524288
    return jax.shard_map(
        functools.partial(body, sizes, total),
        mesh=mesh,
        in_specs=(P("pair", "tm"), P("pair", "tm")),
        out_specs=P("tm", "pair"),
        check_vma=False,
    )
```

```python
import functools
import math

import jax
import jax.numpy as jnp
import ml_dtypes
import numpy as np
from jax import lax
from jax.experimental import pallas as pl
from jax.experimental.pallas import tpu as pltpu
from jax.sharding import PartitionSpec as P

L = 512
BLK = 128
N = 2 * BLK
MESH = pl.DeviceIdType.MESH


def halves(array):
    high = array.astype(ml_dtypes.bfloat16)
    low = (array - high.astype(np.float64)).astype(ml_dtypes.bfloat16)
    return high, low


@functools.cache
def tables(total):
    theta = 2 * np.pi * (np.arange(BLK) + 0.5) / N
    turns = np.outer(np.arange(BLK), theta)
    high, low = halves(np.concatenate([np.cos(turns), np.sin(turns)], axis=1))
    forward = np.stack([np.concatenate([high, high]), np.concatenate([low, low])])
    high, low = halves(np.concatenate([np.cos(turns.T), -np.sin(turns.T)]) * (2.0 / N / math.sqrt(total)))
    return forward, np.concatenate([high, low], axis=1)


def from_far(count):
    return sorted(range(1, count), key=lambda d: -min(d, count - d))


def high_low(value):
    high = value.astype(jnp.bfloat16)
    return high, (value - high.astype(jnp.float32)).astype(jnp.bfloat16)


def kernel(
    sizes, x_hbm, y_hbm, fwd_hbm, bwd_hbm, recv,
    xv, yv, lead, head, fwd, bwd,
    px0, px1, py0, py1, ph0, ph1, fx0, fx1, fy0, fy1, fh0, fh1, res0, res1, split0, split1, send,
    load_sem, halo_sem, send_sem, recv_sem, told,
):
    zs, ys, xs = sizes
    pairs, length = xv.shape
    blocks, extra = length // BLK, L // BLK
    half = pairs // 2
    first, second = slice(0, half), slice(half, pairs)
    group = 2 * ys
    depth = zs // xs
    everyone = zs * group
    last = everyone - 1
    tm, mx = lax.axis_index("tm"), lax.axis_index("pair")
    mz, mg = tm // group, tm % group
    my, mc = mg // 2, mg % 2
    source_x = mz // depth
    own = jnp.where(source_x == mx, 1, 0)

    loads = [
        pltpu.make_async_copy(y_hbm.at[:, 0:L], lead, load_sem.at[0]),
        pltpu.make_async_copy(x_hbm, xv, load_sem.at[1]),
        pltpu.make_async_copy(fwd_hbm, fwd, load_sem.at[2]),
        pltpu.make_async_copy(y_hbm, yv, load_sem.at[3]),
        pltpu.make_async_copy(bwd_hbm, bwd, load_sem.at[4]),
    ]
    for load in loads:
        load.start()

    barrier = pltpu.get_barrier_semaphore()

    def arrived(device, x):
        pl.semaphore_signal(barrier, inc=1, device_id=(device, x), device_id_type=MESH)

    def tell(which, device):
        pl.semaphore_signal(told.at[which], inc=1, device_id=(device, mx), device_id_type=MESH)

    @pl.when(mc == 1)
    def _():
        arrived(tm - 1, mx)

    @pl.when(jnp.logical_and(mc == 1, tm < last))
    def _():
        arrived(tm + 1, mx)

    def greet():
        for d in from_far(zs):
            z = lax.rem(mz + d, zs)
            for y in range(ys):
                arrived(z * group + 2 * y + 1, source_x)
        for d in range(1, ys):
            arrived(mz * group + 2 * lax.rem(my + d, ys) + 1, source_x)

        @pl.when(jnp.logical_or(own == 0, mc == 0))
        def _():
            arrived(mz * group + 2 * my + 1, source_x)

    def transform(values, part, into):
        count = 0
        for value in values:
            for j in range(value.shape[1] // BLK):
                high, low = high_low(value[:, j * BLK : (j + 1) * BLK])
                part[count * half : (count + 1) * half, 0:BLK] = high
                part[count * half : (count + 1) * half, BLK : 2 * BLK] = low
                count += 1
        rows = part[0 : count * half, :]
        into[...] = jnp.dot(rows, fwd[0], preferred_element_type=jnp.float32) + jnp.dot(
            rows, fwd[1], preferred_element_type=jnp.float32
        )

    to_before = pltpu.make_async_remote_copy(
        src_ref=lead,
        dst_ref=head,
        send_sem=halo_sem.at[0],
        recv_sem=halo_sem.at[1],
        device_id=(jnp.maximum(tm - 1, 0), mx),
        device_id_type=MESH,
    )

    greet()

    @pl.when(mc == 0)
    def _():
        pl.semaphore_wait(barrier, 1 + jnp.where(tm > 0, 1, 0))
        tell(0, tm + 1)

    @pl.when(mc == 1)
    def _():
        pl.semaphore_wait(told.at[0], 1)

    loads[0].wait()

    @pl.when(tm > 0)
    def _():
        to_before.start()

    @pl.when(tm == last)
    def _():
        head[...] = jnp.zeros_like(head)

    lane = lax.broadcasted_iota(jnp.int32, (8, BLK), 1)
    sign = jnp.where(lane % 2 == 0, 1.0, -1.0).astype(jnp.float32)

    def take(ref, block, at):
        return (
            ref[block * half + at : block * half + at + 8, 0:BLK],
            ref[block * half + at : block * half + at + 8, BLK : 2 * BLK],
        )

    def turned(value):
        return -sign * value[1], sign * value[0]

    def plus(a, b):
        return b if a is None else (a[0] + b[0], a[1] + b[1])

    def left(x):
        return x[0], x[0] - x[1], x[0] + x[1]

    def right(z):
        return z[0] + z[1], z[1], z[0]

    def add(sums, q, x, z):
        new = [u * v for u, v in zip(x, z)]
        sums[q] = new if sums[q] is None else [u + v for u, v in zip(sums[q], new)]

    def complex_of(sums):
        return [(a - b, c - a) for a, b, c in sums]

    def inner(xs_, ys_, at):
        sums = [None] * extra
        window = {}
        now = take(ys_, 0, at)
        for j in range(blocks - 1):
            ahead = take(ys_, j + 1, at)
            z = right(plus(now, turned(ahead)))
            now = ahead
            window[j] = left(take(xs_, j, at))
            for q in range(min(extra, j + 1)):
                add(sums, q, window[j - q], z)
        return complex_of(sums)

    def outer(xs_, ys_, hs_, at):
        y = [take(ys_, blocks - 1, at)] + [take(hs_, j, at) for j in range(extra)]
        window = [right(plus(y[j], turned(y[j + 1]))) for j in range(extra)]
        sums = [None] * extra
        for b in range(blocks - extra, blocks):
            x = left(take(xs_, b, at))
            for q in range(extra):
                if b + q >= blocks - 1:
                    add(sums, q, x, window[b + q - (blocks - 1)])
        return complex_of(sums)

    def inner_products(xs_, ys_, into):
        for at in range(0, half, 8):
            for q, (real, imag) in enumerate(inner(xs_, ys_, at)):
                rows = slice(q * half + at, q * half + at + 8)
                into[rows, 0:BLK] = real
                into[rows, BLK : 2 * BLK] = imag

    loads[1].wait()
    loads[2].wait()
    transform([xv.at[first]], px0, fx0)

    loads[3].wait()
    loads[4].wait()
    transform([yv.at[first]], py0, fy0)
    transform([xv.at[second]], px1, fx1)
    inner_products(fx0, fy0, res0)
    transform([yv.at[second]], py1, fy1)
    inner_products(fx1, fy1, res1)

    @pl.when(mc == 1)
    def _():
        pl.semaphore_wait(barrier, pairs * xs - own)
        tell(1, tm - 1)

    @pl.when(tm < last)
    def _():
        to_before.wait_recv()

    def finish(base, xs_, ys_, edge, part, hs_, sums, split):
        transform(edge, part, hs_)
        middle = extra * half
        for at in range(0, half, 8):
            for q, values in enumerate(outer(xs_, ys_, hs_, at)):
                rows = slice(q * half + at, q * half + at + 8)
                under = slice(middle + rows.start, middle + rows.stop)
                for which, value in enumerate(values):
                    columns = slice(which * BLK, (which + 1) * BLK)
                    split[rows, columns], split[under, columns] = high_low(
                        sums[rows, columns] + value
                    )
        both = jnp.dot(split[...], bwd[...], preferred_element_type=jnp.float32)
        lagged = (both[0:middle, 0:BLK] + both[0:middle, BLK : 2 * BLK]) + (
            both[middle:, 0:BLK] + both[middle:, BLK : 2 * BLK]
        )
        for q in range(extra):
            send[q * pairs + base : q * pairs + base + half] = lagged[
                q * half : (q + 1) * half
            ].reshape(half, 1, BLK)

    def copy(row, q):
        return pltpu.make_async_remote_copy(
            src_ref=send.at[q * pairs + row],
            dst_ref=recv.at[tm],
            send_sem=send_sem,
            recv_sem=recv_sem,
            device_id=(mx * pairs + row, q),
            device_id_type=MESH,
        )

    own_at = jnp.where(own == 1, tm, -1)
    def send_rows(rows):
        for y in range(ys):
            for row in rows:
                if row // 2 % ys == y:
                    for q in range(xs):

                        @pl.when(own_at != q * pairs + row)
                        def _():
                            copy(row, q).start()

    finish(0, fx0, fy0, [head.at[first]], ph0, fh0, res0, split0)

    @pl.when(mc == 0)
    def _():
        pl.semaphore_wait(told.at[1], 1)

    send_rows(range(half - 1, -1, -1))
    finish(half, fx1, fy1, [head.at[second]], ph1, fh1, res1, split1)
    send_rows(range(pairs - 1, half - 1, -1))

    kept = pltpu.make_async_copy(send.at[tm], recv.at[tm], load_sem.at[5])

    @pl.when(own == 1)
    def _():
        kept.start()

    def all_of(count):
        return pltpu.make_async_remote_copy(
            src_ref=send.at[pl.ds(0, count)],
            dst_ref=recv.at[pl.ds(0, count)],
            send_sem=send_sem,
            recv_sem=recv_sem,
            device_id=(tm, mx),
            device_id_type=MESH,
        )

    for own_too in (0, 1):

        @pl.when(own == own_too)
        def _():
            all_of(everyone - own_too).wait_recv()

    @pl.when(own == 1)
    def _():
        kept.wait()

    @pl.when(tm > 0)
    def _():
        to_before.wait_send()

    for own_too in (0, 1):

        @pl.when(own == own_too)
        def _():
            all_of(everyone - own_too).wait_send()


def body(sizes, total, x_series, y_series):
    fwd, bwd = tables(total)
    zs, ys, xs = sizes
    pairs, length = x_series.shape
    blocks, extra = length // BLK, L // BLK
    f32, bf16 = jnp.float32, jnp.bfloat16
    dma = pltpu.SemaphoreType.DMA
    shares = pl.pallas_call(
        functools.partial(kernel, sizes),
        out_shape=pltpu.VMEM((2 * zs * ys, 1, L // xs), f32),
        in_specs=[pl.BlockSpec(memory_space=pl.ANY)] * 4,
        out_specs=pl.BlockSpec(memory_space=pl.ANY),
        scratch_shapes=[
            pltpu.VMEM((pairs, length), f32),
            pltpu.VMEM((pairs, length), f32),
            pltpu.VMEM((pairs, L), f32),
            pltpu.VMEM((pairs, L), f32),
            pltpu.VMEM(fwd.shape, bf16),
            pltpu.VMEM(bwd.shape, bf16),
            *[pltpu.VMEM((blocks * pairs // 2, 2 * BLK), bf16)] * 4,
            *[pltpu.VMEM((extra * pairs // 2, 2 * BLK), bf16)] * 2,
            *[pltpu.VMEM((blocks * pairs // 2, N), f32)] * 4,
            *[pltpu.VMEM((extra * pairs // 2, N), f32)] * 2,
            *[pltpu.VMEM((extra * pairs // 2, N), f32)] * 2,
            *[pltpu.VMEM((extra * pairs, N), bf16)] * 2,
            pltpu.VMEM((pairs * xs, 1, L // xs), f32),
            dma((6,)),
            dma((2,)),
            dma,
            dma,
            pltpu.SemaphoreType.REGULAR((2,)),
        ],
        compiler_params=pltpu.CompilerParams(collective_id=0, has_side_effects=True),
    )(x_series, y_series, jnp.asarray(fwd), jnp.asarray(bwd))
    return jnp.sum(shares, axis=0)


def solution(mesh):
    sizes = (8, 8, mesh.shape["pair"])
    total = 524288
    return jax.shard_map(
        functools.partial(body, sizes, total),
        mesh=mesh,
        in_specs=(P("pair", "tm"), P("pair", "tm")),
        out_specs=P("tm", "pair"),
        check_vma=False,
    )
```

```python
import functools
import math

import jax
import jax.numpy as jnp
import ml_dtypes
import numpy as np
from jax import lax
from jax.experimental import pallas as pl
from jax.experimental.pallas import tpu as pltpu
from jax.sharding import PartitionSpec as P

L = 512
BLK = 128
N = 2 * BLK
MESH = pl.DeviceIdType.MESH


def halves(array):
    high = array.astype(ml_dtypes.bfloat16)
    low = (array - high.astype(np.float64)).astype(ml_dtypes.bfloat16)
    return high, low


@functools.cache
def tables(total):
    theta = 2 * np.pi * (np.arange(BLK) + 0.5) / N
    turns = np.outer(np.arange(BLK), theta)
    high, low = halves(np.concatenate([np.cos(turns), np.sin(turns)], axis=1))
    forward = np.stack([np.concatenate([high, high]), np.concatenate([low, low])])
    high, low = halves(np.concatenate([np.cos(turns.T), -np.sin(turns.T)]) * (2.0 / N / math.sqrt(total)))
    return forward, np.concatenate([high, low], axis=1)


def from_far(count):
    return sorted(range(1, count), key=lambda d: -min(d, count - d))


def high_low(value):
    high = value.astype(jnp.bfloat16)
    return high, (value - high.astype(jnp.float32)).astype(jnp.bfloat16)


def kernel(
    sizes, x_hbm, y_hbm, fwd_hbm, bwd_hbm, recv,
    xv, yv, lead, head, fwd, bwd,
    px0, px1, py0, py1, ph0, ph1, fx0, fx1, fy0, fy1, fh0, fh1, res0, res1, split0, split1, send,
    load_sem, halo_sem, send_sem, recv_sem, told,
):
    zs, ys, xs = sizes
    pairs, length = xv.shape
    blocks, extra = length // BLK, L // BLK
    half = pairs // 2
    first, second = slice(0, half), slice(half, pairs)
    group = 2 * ys
    depth = zs // xs
    everyone = zs * group
    last = everyone - 1
    tm, mx = lax.axis_index("tm"), lax.axis_index("pair")
    mz, mg = tm // group, tm % group
    my, mc = mg // 2, mg % 2
    source_x = mz // depth
    own = jnp.where(source_x == mx, 1, 0)

    loads = [
        pltpu.make_async_copy(y_hbm.at[:, 0:L], lead, load_sem.at[0]),
        pltpu.make_async_copy(x_hbm, xv, load_sem.at[1]),
        pltpu.make_async_copy(fwd_hbm, fwd, load_sem.at[2]),
        pltpu.make_async_copy(y_hbm, yv, load_sem.at[3]),
        pltpu.make_async_copy(bwd_hbm, bwd, load_sem.at[4]),
    ]
    for load in loads:
        load.start()

    barrier = pltpu.get_barrier_semaphore()

    def arrived(device, x):
        pl.semaphore_signal(barrier, inc=1, device_id=(device, x), device_id_type=MESH)

    def tell(which, device):
        pl.semaphore_signal(told.at[which], inc=1, device_id=(device, mx), device_id_type=MESH)

    @pl.when(mc == 1)
    def _():
        arrived(tm - 1, mx)

    @pl.when(jnp.logical_and(mc == 1, tm < last))
    def _():
        arrived(tm + 1, mx)

    def greet():
        for d in from_far(zs):
            z = lax.rem(mz + d, zs)
            for y in range(ys):
                arrived(z * group + 2 * y + 1, source_x)
        for d in range(1, ys):
            arrived(mz * group + 2 * lax.rem(my + d, ys) + 1, source_x)

        @pl.when(jnp.logical_or(own == 0, mc == 0))
        def _():
            arrived(mz * group + 2 * my + 1, source_x)

    def transform(values, part, into):
        count = 0
        for value in values:
            for j in range(value.shape[1] // BLK):
                high, low = high_low(value[:, j * BLK : (j + 1) * BLK])
                part[count * half : (count + 1) * half, 0:BLK] = high
                part[count * half : (count + 1) * half, BLK : 2 * BLK] = low
                count += 1
        rows = part[0 : count * half, :]
        into[...] = jnp.dot(rows, fwd[0], preferred_element_type=jnp.float32) + jnp.dot(
            rows, fwd[1], preferred_element_type=jnp.float32
        )

    to_before = [
        pltpu.make_async_remote_copy(
            src_ref=lead.at[rows],
            dst_ref=head.at[rows],
            send_sem=halo_sem.at[i],
            recv_sem=halo_sem.at[2 + i],
            device_id=(jnp.maximum(tm - 1, 0), mx),
            device_id_type=MESH,
        )
        for i, rows in enumerate((first, second))
    ]

    greet()

    @pl.when(mc == 0)
    def _():
        pl.semaphore_wait(barrier, 1 + jnp.where(tm > 0, 1, 0))
        tell(0, tm + 1)

    @pl.when(mc == 1)
    def _():
        pl.semaphore_wait(told.at[0], 1)

    loads[0].wait()

    @pl.when(tm > 0)
    def _():
        for part in to_before:
            part.start()

    @pl.when(tm == last)
    def _():
        head[...] = jnp.zeros_like(head)

    lane = lax.broadcasted_iota(jnp.int32, (8, BLK), 1)
    sign = jnp.where(lane % 2 == 0, 1.0, -1.0).astype(jnp.float32)

    def take(ref, block, at):
        return (
            ref[block * half + at : block * half + at + 8, 0:BLK],
            ref[block * half + at : block * half + at + 8, BLK : 2 * BLK],
        )

    def turned(value):
        return -sign * value[1], sign * value[0]

    def plus(a, b):
        return b if a is None else (a[0] + b[0], a[1] + b[1])

    def left(x):
        return x[0], x[0] - x[1], x[0] + x[1]

    def right(z):
        return z[0] + z[1], z[1], z[0]

    def add(sums, q, x, z):
        new = [u * v for u, v in zip(x, z)]
        sums[q] = new if sums[q] is None else [u + v for u, v in zip(sums[q], new)]

    def complex_of(sums):
        return [(a - b, c - a) for a, b, c in sums]

    def inner(xs_, ys_, at):
        sums = [None] * extra
        window = {}
        now = take(ys_, 0, at)
        for j in range(blocks - 1):
            ahead = take(ys_, j + 1, at)
            z = right(plus(now, turned(ahead)))
            now = ahead
            window[j] = left(take(xs_, j, at))
            for q in range(min(extra, j + 1)):
                add(sums, q, window[j - q], z)
        return complex_of(sums)

    def outer(xs_, ys_, hs_, at):
        y = [take(ys_, blocks - 1, at)] + [take(hs_, j, at) for j in range(extra)]
        window = [right(plus(y[j], turned(y[j + 1]))) for j in range(extra)]
        sums = [None] * extra
        for b in range(blocks - extra, blocks):
            x = left(take(xs_, b, at))
            for q in range(extra):
                if b + q >= blocks - 1:
                    add(sums, q, x, window[b + q - (blocks - 1)])
        return complex_of(sums)

    def inner_products(xs_, ys_, into):
        for at in range(0, half, 8):
            for q, (real, imag) in enumerate(inner(xs_, ys_, at)):
                rows = slice(q * half + at, q * half + at + 8)
                into[rows, 0:BLK] = real
                into[rows, BLK : 2 * BLK] = imag

    loads[1].wait()
    loads[2].wait()
    transform([xv.at[first]], px0, fx0)

    loads[3].wait()
    loads[4].wait()
    transform([yv.at[first]], py0, fy0)
    transform([xv.at[second]], px1, fx1)
    inner_products(fx0, fy0, res0)
    transform([yv.at[second]], py1, fy1)
    inner_products(fx1, fy1, res1)

    @pl.when(mc == 1)
    def _():
        pl.semaphore_wait(barrier, pairs * xs - own)
        tell(1, tm - 1)

    def finish(base, xs_, ys_, edge, part, hs_, sums, split):
        transform(edge, part, hs_)
        middle = extra * half
        for at in range(0, half, 8):
            for q, values in enumerate(outer(xs_, ys_, hs_, at)):
                rows = slice(q * half + at, q * half + at + 8)
                under = slice(middle + rows.start, middle + rows.stop)
                for which, value in enumerate(values):
                    columns = slice(which * BLK, (which + 1) * BLK)
                    split[rows, columns], split[under, columns] = high_low(
                        sums[rows, columns] + value
                    )
        both = jnp.dot(split[...], bwd[...], preferred_element_type=jnp.float32)
        lagged = (both[0:middle, 0:BLK] + both[0:middle, BLK : 2 * BLK]) + (
            both[middle:, 0:BLK] + both[middle:, BLK : 2 * BLK]
        )
        for q in range(extra):
            send[q * pairs + base : q * pairs + base + half] = lagged[
                q * half : (q + 1) * half
            ].reshape(half, 1, BLK)

    def copy(row, q):
        return pltpu.make_async_remote_copy(
            src_ref=send.at[q * pairs + row],
            dst_ref=recv.at[tm],
            send_sem=send_sem,
            recv_sem=recv_sem,
            device_id=(mx * pairs + row, q),
            device_id_type=MESH,
        )

    own_at = jnp.where(own == 1, tm, -1)
    def send_rows(rows):
        for y in range(ys):
            for row in rows:
                if row // 2 % ys == y:
                    for q in range(xs):

                        @pl.when(own_at != q * pairs + row)
                        def _():
                            copy(row, q).start()

    @pl.when(tm < last)
    def _():
        to_before[0].wait_recv()

    finish(0, fx0, fy0, [head.at[first]], ph0, fh0, res0, split0)

    @pl.when(mc == 0)
    def _():
        pl.semaphore_wait(told.at[1], 1)

    send_rows(range(half - 1, -1, -1))
    @pl.when(tm < last)
    def _():
        to_before[1].wait_recv()

    finish(half, fx1, fy1, [head.at[second]], ph1, fh1, res1, split1)
    send_rows(range(pairs - 1, half - 1, -1))

    kept = pltpu.make_async_copy(send.at[tm], recv.at[tm], load_sem.at[5])

    @pl.when(own == 1)
    def _():
        kept.start()

    def all_of(count):
        return pltpu.make_async_remote_copy(
            src_ref=send.at[pl.ds(0, count)],
            dst_ref=recv.at[pl.ds(0, count)],
            send_sem=send_sem,
            recv_sem=recv_sem,
            device_id=(tm, mx),
            device_id_type=MESH,
        )

    for own_too in (0, 1):

        @pl.when(own == own_too)
        def _():
            all_of(everyone - own_too).wait_recv()

    @pl.when(own == 1)
    def _():
        kept.wait()

    @pl.when(tm > 0)
    def _():
        for part in to_before:
            part.wait_send()

    for own_too in (0, 1):

        @pl.when(own == own_too)
        def _():
            all_of(everyone - own_too).wait_send()


def body(sizes, total, x_series, y_series):
    fwd, bwd = tables(total)
    zs, ys, xs = sizes
    pairs, length = x_series.shape
    blocks, extra = length // BLK, L // BLK
    f32, bf16 = jnp.float32, jnp.bfloat16
    dma = pltpu.SemaphoreType.DMA
    shares = pl.pallas_call(
        functools.partial(kernel, sizes),
        out_shape=pltpu.VMEM((2 * zs * ys, 1, L // xs), f32),
        in_specs=[pl.BlockSpec(memory_space=pl.ANY)] * 4,
        out_specs=pl.BlockSpec(memory_space=pl.ANY),
        scratch_shapes=[
            pltpu.VMEM((pairs, length), f32),
            pltpu.VMEM((pairs, length), f32),
            pltpu.VMEM((pairs, L), f32),
            pltpu.VMEM((pairs, L), f32),
            pltpu.VMEM(fwd.shape, bf16),
            pltpu.VMEM(bwd.shape, bf16),
            *[pltpu.VMEM((blocks * pairs // 2, 2 * BLK), bf16)] * 4,
            *[pltpu.VMEM((extra * pairs // 2, 2 * BLK), bf16)] * 2,
            *[pltpu.VMEM((blocks * pairs // 2, N), f32)] * 4,
            *[pltpu.VMEM((extra * pairs // 2, N), f32)] * 2,
            *[pltpu.VMEM((extra * pairs // 2, N), f32)] * 2,
            *[pltpu.VMEM((extra * pairs, N), bf16)] * 2,
            pltpu.VMEM((pairs * xs, 1, L // xs), f32),
            dma((6,)),
            dma((4,)),
            dma,
            dma,
            pltpu.SemaphoreType.REGULAR((2,)),
        ],
        compiler_params=pltpu.CompilerParams(collective_id=0, has_side_effects=True),
    )(x_series, y_series, jnp.asarray(fwd), jnp.asarray(bwd))
    return jnp.sum(shares, axis=0)


def solution(mesh):
    sizes = (8, 8, mesh.shape["pair"])
    total = 524288
    return jax.shard_map(
        functools.partial(body, sizes, total),
        mesh=mesh,
        in_specs=(P("pair", "tm"), P("pair", "tm")),
        out_specs=P("tm", "pair"),
        check_vma=False,
    )
```

```python
import functools
import math

import jax
import jax.numpy as jnp
import ml_dtypes
import numpy as np
from jax import lax
from jax.experimental import pallas as pl
from jax.experimental.pallas import tpu as pltpu
from jax.sharding import PartitionSpec as P

L = 512
BLK = 128
N = 2 * BLK
MESH = pl.DeviceIdType.MESH


def halves(array):
    high = array.astype(ml_dtypes.bfloat16)
    low = (array - high.astype(np.float64)).astype(ml_dtypes.bfloat16)
    return high, low


@functools.cache
def tables(total):
    theta = 2 * np.pi * (np.arange(BLK) + 0.5) / N
    turns = np.outer(np.arange(BLK), theta)
    high, low = halves(np.concatenate([np.cos(turns), np.sin(turns)], axis=1))
    forward = np.stack([np.concatenate([high, high]), np.concatenate([low, low])])
    high, low = halves(np.concatenate([np.cos(turns.T), -np.sin(turns.T)]) * (2.0 / N / math.sqrt(total)))
    return forward, np.concatenate([high, low], axis=1)


def from_far(count):
    return sorted(range(1, count), key=lambda d: -min(d, count - d))


def high_low(value):
    high = value.astype(jnp.bfloat16)
    return high, (value - high.astype(jnp.float32)).astype(jnp.bfloat16)


def kernel(
    sizes, x_hbm, y_hbm, fwd_hbm, bwd_hbm, recv,
    xv, yv, lead, head, fwd, bwd,
    px0, px1, py0, py1, ph0, ph1, fx0, fx1, fy0, fy1, fh0, fh1, res0, res1, split0, split1, send,
    load_sem, halo_sem, send_sem, recv_sem, told,
):
    zs, ys, xs = sizes
    pairs, length = xv.shape
    blocks, extra = length // BLK, L // BLK
    half = pairs // 2
    first, second = slice(0, half), slice(half, pairs)
    group = 2 * ys
    depth = zs // xs
    everyone = zs * group
    last = everyone - 1
    tm, mx = lax.axis_index("tm"), lax.axis_index("pair")
    mz, mg = tm // group, tm % group
    my, mc = mg // 2, mg % 2
    source_x = mz // depth
    own = jnp.where(source_x == mx, 1, 0)

    loads = [
        pltpu.make_async_copy(y_hbm.at[first, 0:L], lead.at[first], load_sem.at[0]),
        pltpu.make_async_copy(x_hbm, xv, load_sem.at[1]),
        pltpu.make_async_copy(fwd_hbm, fwd, load_sem.at[2]),
        pltpu.make_async_copy(y_hbm, yv, load_sem.at[3]),
        pltpu.make_async_copy(bwd_hbm, bwd, load_sem.at[4]),
        pltpu.make_async_copy(y_hbm.at[second, 0:L], lead.at[second], load_sem.at[6]),
    ]
    for i in (0, 5, 1, 2, 3, 4):
        loads[i].start()

    barrier = pltpu.get_barrier_semaphore()

    def arrived(device, x):
        pl.semaphore_signal(barrier, inc=1, device_id=(device, x), device_id_type=MESH)

    def tell(which, device):
        pl.semaphore_signal(told.at[which], inc=1, device_id=(device, mx), device_id_type=MESH)

    @pl.when(mc == 1)
    def _():
        arrived(tm - 1, mx)

    @pl.when(jnp.logical_and(mc == 1, tm < last))
    def _():
        arrived(tm + 1, mx)

    def greet():
        for d in from_far(zs):
            z = lax.rem(mz + d, zs)
            for y in range(ys):
                arrived(z * group + 2 * y + 1, source_x)
        for d in range(1, ys):
            arrived(mz * group + 2 * lax.rem(my + d, ys) + 1, source_x)

        @pl.when(jnp.logical_or(own == 0, mc == 0))
        def _():
            arrived(mz * group + 2 * my + 1, source_x)

    def transform(values, part, into):
        count = 0
        for value in values:
            for j in range(value.shape[1] // BLK):
                high, low = high_low(value[:, j * BLK : (j + 1) * BLK])
                part[count * half : (count + 1) * half, 0:BLK] = high
                part[count * half : (count + 1) * half, BLK : 2 * BLK] = low
                count += 1
        rows = part[0 : count * half, :]
        into[...] = jnp.dot(rows, fwd[0], preferred_element_type=jnp.float32) + jnp.dot(
            rows, fwd[1], preferred_element_type=jnp.float32
        )

    to_before = [
        pltpu.make_async_remote_copy(
            src_ref=lead.at[rows],
            dst_ref=head.at[rows],
            send_sem=halo_sem.at[i],
            recv_sem=halo_sem.at[2 + i],
            device_id=(jnp.maximum(tm - 1, 0), mx),
            device_id_type=MESH,
        )
        for i, rows in enumerate((first, second))
    ]

    greet()

    @pl.when(mc == 0)
    def _():
        pl.semaphore_wait(barrier, 1 + jnp.where(tm > 0, 1, 0))
        tell(0, tm + 1)

    @pl.when(mc == 1)
    def _():
        pl.semaphore_wait(told.at[0], 1)

    for load, part in ((loads[0], to_before[0]), (loads[5], to_before[1])):
        load.wait()

        @pl.when(tm > 0)
        def _():
            part.start()

    @pl.when(tm == last)
    def _():
        head[...] = jnp.zeros_like(head)

    lane = lax.broadcasted_iota(jnp.int32, (8, BLK), 1)
    sign = jnp.where(lane % 2 == 0, 1.0, -1.0).astype(jnp.float32)

    def take(ref, block, at):
        return (
            ref[block * half + at : block * half + at + 8, 0:BLK],
            ref[block * half + at : block * half + at + 8, BLK : 2 * BLK],
        )

    def turned(value):
        return -sign * value[1], sign * value[0]

    def plus(a, b):
        return b if a is None else (a[0] + b[0], a[1] + b[1])

    def left(x):
        return x[0], x[0] - x[1], x[0] + x[1]

    def right(z):
        return z[0] + z[1], z[1], z[0]

    def add(sums, q, x, z):
        new = [u * v for u, v in zip(x, z)]
        sums[q] = new if sums[q] is None else [u + v for u, v in zip(sums[q], new)]

    def complex_of(sums):
        return [(a - b, c - a) for a, b, c in sums]

    def inner(xs_, ys_, at):
        sums = [None] * extra
        window = {}
        now = take(ys_, 0, at)
        for j in range(blocks - 1):
            ahead = take(ys_, j + 1, at)
            z = right(plus(now, turned(ahead)))
            now = ahead
            window[j] = left(take(xs_, j, at))
            for q in range(min(extra, j + 1)):
                add(sums, q, window[j - q], z)
        return complex_of(sums)

    def outer(xs_, ys_, hs_, at):
        y = [take(ys_, blocks - 1, at)] + [take(hs_, j, at) for j in range(extra)]
        window = [right(plus(y[j], turned(y[j + 1]))) for j in range(extra)]
        sums = [None] * extra
        for b in range(blocks - extra, blocks):
            x = left(take(xs_, b, at))
            for q in range(extra):
                if b + q >= blocks - 1:
                    add(sums, q, x, window[b + q - (blocks - 1)])
        return complex_of(sums)

    def inner_products(xs_, ys_, into):
        for at in range(0, half, 8):
            for q, (real, imag) in enumerate(inner(xs_, ys_, at)):
                rows = slice(q * half + at, q * half + at + 8)
                into[rows, 0:BLK] = real
                into[rows, BLK : 2 * BLK] = imag

    loads[1].wait()
    loads[2].wait()
    transform([xv.at[first]], px0, fx0)

    loads[3].wait()
    loads[4].wait()
    transform([yv.at[first]], py0, fy0)
    transform([xv.at[second]], px1, fx1)
    inner_products(fx0, fy0, res0)
    transform([yv.at[second]], py1, fy1)
    inner_products(fx1, fy1, res1)

    @pl.when(mc == 1)
    def _():
        pl.semaphore_wait(barrier, pairs * xs - own)
        tell(1, tm - 1)

    def finish(base, xs_, ys_, edge, part, hs_, sums, split):
        transform(edge, part, hs_)
        middle = extra * half
        for at in range(0, half, 8):
            for q, values in enumerate(outer(xs_, ys_, hs_, at)):
                rows = slice(q * half + at, q * half + at + 8)
                under = slice(middle + rows.start, middle + rows.stop)
                for which, value in enumerate(values):
                    columns = slice(which * BLK, (which + 1) * BLK)
                    split[rows, columns], split[under, columns] = high_low(
                        sums[rows, columns] + value
                    )
        both = jnp.dot(split[...], bwd[...], preferred_element_type=jnp.float32)
        lagged = (both[0:middle, 0:BLK] + both[0:middle, BLK : 2 * BLK]) + (
            both[middle:, 0:BLK] + both[middle:, BLK : 2 * BLK]
        )
        for q in range(extra):
            send[q * pairs + base : q * pairs + base + half] = lagged[
                q * half : (q + 1) * half
            ].reshape(half, 1, BLK)

    def copy(row, q):
        return pltpu.make_async_remote_copy(
            src_ref=send.at[q * pairs + row],
            dst_ref=recv.at[tm],
            send_sem=send_sem,
            recv_sem=recv_sem,
            device_id=(mx * pairs + row, q),
            device_id_type=MESH,
        )

    own_at = jnp.where(own == 1, tm, -1)
    def send_rows(rows):
        for y in range(ys):
            for row in rows:
                if row // 2 % ys == y:
                    for q in range(xs):

                        @pl.when(own_at != q * pairs + row)
                        def _():
                            copy(row, q).start()

    @pl.when(tm < last)
    def _():
        to_before[0].wait_recv()

    finish(0, fx0, fy0, [head.at[first]], ph0, fh0, res0, split0)

    @pl.when(mc == 0)
    def _():
        pl.semaphore_wait(told.at[1], 1)

    send_rows(range(half - 1, -1, -1))
    @pl.when(tm < last)
    def _():
        to_before[1].wait_recv()

    finish(half, fx1, fy1, [head.at[second]], ph1, fh1, res1, split1)
    send_rows(range(pairs - 1, half - 1, -1))

    kept = pltpu.make_async_copy(send.at[tm], recv.at[tm], load_sem.at[5])

    @pl.when(own == 1)
    def _():
        kept.start()

    def all_of(count):
        return pltpu.make_async_remote_copy(
            src_ref=send.at[pl.ds(0, count)],
            dst_ref=recv.at[pl.ds(0, count)],
            send_sem=send_sem,
            recv_sem=recv_sem,
            device_id=(tm, mx),
            device_id_type=MESH,
        )

    for own_too in (0, 1):

        @pl.when(own == own_too)
        def _():
            all_of(everyone - own_too).wait_recv()

    @pl.when(own == 1)
    def _():
        kept.wait()

    @pl.when(tm > 0)
    def _():
        for part in to_before:
            part.wait_send()

    for own_too in (0, 1):

        @pl.when(own == own_too)
        def _():
            all_of(everyone - own_too).wait_send()


def body(sizes, total, x_series, y_series):
    fwd, bwd = tables(total)
    zs, ys, xs = sizes
    pairs, length = x_series.shape
    blocks, extra = length // BLK, L // BLK
    f32, bf16 = jnp.float32, jnp.bfloat16
    dma = pltpu.SemaphoreType.DMA
    shares = pl.pallas_call(
        functools.partial(kernel, sizes),
        out_shape=pltpu.VMEM((2 * zs * ys, 1, L // xs), f32),
        in_specs=[pl.BlockSpec(memory_space=pl.ANY)] * 4,
        out_specs=pl.BlockSpec(memory_space=pl.ANY),
        scratch_shapes=[
            pltpu.VMEM((pairs, length), f32),
            pltpu.VMEM((pairs, length), f32),
            pltpu.VMEM((pairs, L), f32),
            pltpu.VMEM((pairs, L), f32),
            pltpu.VMEM(fwd.shape, bf16),
            pltpu.VMEM(bwd.shape, bf16),
            *[pltpu.VMEM((blocks * pairs // 2, 2 * BLK), bf16)] * 4,
            *[pltpu.VMEM((extra * pairs // 2, 2 * BLK), bf16)] * 2,
            *[pltpu.VMEM((blocks * pairs // 2, N), f32)] * 4,
            *[pltpu.VMEM((extra * pairs // 2, N), f32)] * 2,
            *[pltpu.VMEM((extra * pairs // 2, N), f32)] * 2,
            *[pltpu.VMEM((extra * pairs, N), bf16)] * 2,
            pltpu.VMEM((pairs * xs, 1, L // xs), f32),
            dma((7,)),
            dma((4,)),
            dma,
            dma,
            pltpu.SemaphoreType.REGULAR((2,)),
        ],
        compiler_params=pltpu.CompilerParams(collective_id=0, has_side_effects=True),
    )(x_series, y_series, jnp.asarray(fwd), jnp.asarray(bwd))
    return jnp.sum(shares, axis=0)


def solution(mesh):
    sizes = (8, 8, mesh.shape["pair"])
    total = 524288
    return jax.shard_map(
        functools.partial(body, sizes, total),
        mesh=mesh,
        in_specs=(P("pair", "tm"), P("pair", "tm")),
        out_specs=P("tm", "pair"),
        check_vma=False,
    )
```
